32 devices in a mesh: sky: 8 (over z, y), band: 4 (over x, core).
Axes of the slice: x: 2, y: 2, z: 4, core: 2. Of those that a mesh axis runs over, the one named last changes fastest.
Arguments:
- magnitudes: float32 [4, 8, 16384], P('band', None, 'sky'), may hold values from -7 to 7
- weights: float32 [4, 8, 16384], P('band', None, 'sky'), may hold values from 0.25 to 4
- slots: int32 [4, 8, 16384], P('band', None, 'sky'), may hold values from 0 to 31, as said below
- block_fields: int32 [64, 32], P('sky'), may hold values from 0 to 4096, as said below
- owner: int32 [4096], replicated, may hold values from 0 to 7, as said below
- colors: int32 [4096], replicated, may hold values from 0 to 7
- color_terms: float32 [4, 4], replicated, may hold values from -0.25 to 0.25
Outputs:
- zero_points: float32 [4, 4096], P('band', 'sky')
- star_mags: float32 [4, 16384], P('band', 'sky')
- misfit: float32 [4, 4], P(None, 'band')
The draws below stay inside these ranges and needn't reach their ends.
Inputs may be any that keep to these rules, and one draw needn't show every extreme that they name: `block_fields`: the live entries of each list come first, are distinct, and name fields owned by the block's own sky tile or by the tiles one index below or above it, cyclically over 8 tiles; the remaining entries equal 4096. A list holds 16 or more live entries, and every tile has a block with all 32 live. `owner`: each sky tile owns exactly 512 fields. `slots`: each observation names a live entry of its block's list.
All inputs are finite; a program needn't handle non-finite values.
Results may differ from the reference program's by a relative error of at most 0.00023.
Values sent between devices are 32-bit elements; how exact they have to be, the bound alone decides.
No kernel may reach another device: no remote copies, remote signals or barrier semaphores. Data moves between devices by JAX's collectives and lax.ppermute only.
A program may use at most 64 MiB of HBM per device.

```python
import math
import jax
import jax.numpy as jnp
from jax import lax

F = 4096
COLORS = 8
SWEEPS = 4
OBS = 8
LIST = 32
ROWS = 256
BLK_DEV = 8
NBANDS = 4
TILES = 8
F_OWN = 512
NBLOCKS = 64
NSTARS = 16384


def layout(key):
    permuted = jax.random.permutation(jax.random.fold_in(key, 1), F)
    owner = (permuted // F_OWN).astype(jnp.int32)
    inverse = jnp.argsort(permuted, stable=True)
    tile_of = jnp.arange(NBLOCKS) // BLK_DEV
    offsets = jnp.arange(3 * F_OWN)
    nearby = (tile_of[:, None] + offsets[None, :] // F_OWN - 1) % TILES * F_OWN + offsets[None, :] % F_OWN
    candidates = inverse[nearby]
    pick_keys = jax.random.split(jax.random.fold_in(key, 2), NBLOCKS)
    shuffles = jax.vmap(lambda block_key: jax.random.permutation(block_key, 3 * F_OWN))(pick_keys)[:, :LIST]
    picked = jnp.take_along_axis(candidates, shuffles, axis=1)
    live_count = jax.random.randint(jax.random.fold_in(key, 3), (NBLOCKS,), LIST // 2, LIST + 1)
    full_block = tile_of * BLK_DEV + tile_of * 5 % BLK_DEV
    live_count = live_count.at[full_block].set(LIST)
    lists = jnp.where(jnp.arange(LIST)[None, :] < live_count[:, None], picked, F).astype(jnp.int32)
    raw_bits = jax.random.randint(jax.random.fold_in(key, 4), (NBANDS, OBS, NSTARS), 0, 1 << 20)
    star_live = jnp.repeat(live_count, ROWS)
    slot_values = (raw_bits % star_live[None, None, :]).astype(jnp.int32)
    return (owner, lists, slot_values)


def draw_block_fields(key, part):
    return layout(key)[1]


def draw_owner(key, part):
    return layout(key)[0]


def draw_slots(key, part):
    return layout(key)[2]


def draw_magnitudes(key, part):
    owner, lists, slot_values = layout(key)
    expanded = jnp.broadcast_to(lists[None, None, :, :], (NBANDS, OBS, NBLOCKS, LIST))
    field_ids = jnp.take_along_axis(expanded, slot_values.reshape(NBANDS, OBS, NBLOCKS, ROWS), axis=3).reshape(NBANDS, OBS, NSTARS)
    star_tint = jax.random.uniform(jax.random.fold_in(key, 11), (NSTARS,), jnp.float32, -1.0, 1.0)
    band_slope = jax.random.uniform(jax.random.fold_in(key, 12), (NBANDS,), jnp.float32, -1.0, 1.0)
    base_mag = jax.random.uniform(jax.random.fold_in(key, 13), (NSTARS,), jnp.float32, -3.0, 3.0)
    field_off = jax.random.uniform(jax.random.fold_in(key, 14), (NBANDS, F), jnp.float32, -1.0, 1.0)
    noise_term = 0.05 * jnp.clip(jax.random.normal(jax.random.fold_in(key, 15), (NBANDS, OBS, NSTARS), jnp.float32), -2.0, 2.0)
    star_part = base_mag[None, :] + band_slope[:, None] * star_tint[None, :]
    field_part = jax.vmap(jnp.take)(field_off, field_ids)
    return (star_part[:, None, :] + field_part + noise_term).astype(jnp.float32)


def place_ends(result, own_key, least, largest):
    place = [jax.random.randint(jax.random.fold_in(own_key, axis), (), 0, length) for axis, length in enumerate(result.shape)]
    widest = result.shape.index(max(result.shape))
    next_to = place[:widest] + [(place[widest] + 1) % result.shape[widest]] + place[widest + 1:]
    return result.at[tuple(place)].set(least).at[tuple(next_to)].set(largest)


def block_scale(stream_key, extent, cuts, smallest, largest):
    gain, own = 1.0, jax.random.fold_in(stream_key, 6)
    for position, blocks in cuts:
        draws = jnp.exp(jax.random.uniform(jax.random.fold_in(own, position), (blocks,), jnp.float32, smallest / len(cuts), largest / len(cuts)))
        gain = gain * jnp.repeat(draws, extent[position] // blocks).reshape([-1 if axis == position else 1 for axis in range(len(extent))])
    return gain


def setup_inputs(seed: int = 0) -> dict:
    seeds = jax.random.split(jax.random.key(seed), 8)
    magnitudes = draw_magnitudes(jax.random.fold_in(seeds[7], 71), 0)
    weights = jnp.clip(jnp.exp(math.log(4.0) - 2.7725887 * jax.random.uniform(seeds[1], (NBANDS, OBS, NSTARS), jnp.float32) ** block_scale(seeds[1], (NBANDS, OBS, NSTARS), ((0, 4), (2, 8)), -0.2, 0.2)), 0.25, 4.0)
    slots = draw_slots(jax.random.fold_in(seeds[7], 71), 0)
    block_fields = draw_block_fields(jax.random.fold_in(seeds[7], 71), 0)
    owner = draw_owner(jax.random.fold_in(seeds[7], 71), 0)
    colors = place_ends(jax.random.randint(seeds[5], (F,), 0, COLORS), jax.random.fold_in(seeds[5], 1), 0, COLORS - 1).astype(jnp.int32)
    color_terms = jnp.clip(jax.random.uniform(seeds[6], (NBANDS, NBANDS), jnp.float32, -0.25, 0.25), -0.25, 0.25)
    return {"magnitudes": magnitudes, "weights": weights, "slots": slots, "block_fields": block_fields, "owner": owner, "colors": colors, "color_terms": color_terms}


PRIOR_WEIGHT = 1.0


def field_table(block_fields, slots):
    band_count, obs_count, star_count = slots.shape
    block_count, list_len = block_fields.shape
    block_rows = star_count // block_count
    block_slots = slots.reshape(band_count, obs_count, block_count, block_rows)
    expanded = jnp.broadcast_to(block_fields[None, None, :, :], (band_count, obs_count, block_count, list_len))
    picked = jnp.take_along_axis(expanded, block_slots, axis=3)
    return picked.reshape(band_count, obs_count, star_count).astype(jnp.int32)


def reference(magnitudes, weights, slots, block_fields, owner, colors, color_terms):
    band_count, obs_count, star_count = magnitudes.shape
    fields = owner.shape[0]
    field_ids = field_table(block_fields, slots)
    star_weight = jnp.sum(weights, axis=1)

    def segment_one(band_values, band_ids):
        return jax.ops.segment_sum(band_values.reshape(-1), band_ids.reshape(-1), num_segments=fields)

    def field_sums(values):
        return jax.vmap(segment_one)(values, field_ids)

    denominators = field_sums(weights) + PRIOR_WEIGHT
    mixing = jnp.eye(band_count, dtype=jnp.float32) + color_terms - jnp.diag(jnp.sum(color_terms, axis=1))

    def predict(zero_pts):
        zp_obs = jax.vmap(jnp.take)(zero_pts, field_ids)
        star_means = jnp.sum(weights * (magnitudes - zp_obs), axis=1) / star_weight
        predicted = jnp.dot(mixing, star_means, precision=lax.Precision.HIGHEST)
        return zp_obs, star_means, predicted

    zero_pts = jnp.zeros((band_count, fields), jnp.float32)
    misfits = []
    for sweep_no in range(SWEEPS):
        for color_no in range(COLORS):
            zp_obs, star_means, predicted = predict(zero_pts)
            residual = magnitudes - predicted[:, None, :]
            if color_no == 0 and sweep_no > 0:
                misfits.append(jnp.sum(weights * (residual - zp_obs) ** 2, axis=(1, 2)))
            updated = field_sums(weights * residual) / denominators
            zero_pts = jnp.where((colors == color_no)[None, :], updated, zero_pts)
    zp_obs, star_means, predicted = predict(zero_pts)
    residual = magnitudes - predicted[:, None, :]
    misfits.append(jnp.sum(weights * (residual - zp_obs) ** 2, axis=(1, 2)))
    misfit = jnp.stack(misfits) / (obs_count * star_count)
    owner_order = jnp.argsort(owner, stable=True)
    return jnp.take(zero_pts, owner_order, axis=1), star_means, misfit
```

```python
import functools

import jax
import jax.numpy as jnp
from jax import lax
from jax.experimental import pallas as pl
from jax.experimental.pallas import tpu as pltpu
from jax.sharding import PartitionSpec as P

COLORS = 8
SWEEPS = 4


PRIOR_WEIGHT = 1.0
LANES = 128
SUBS = 8
HALF = LANES // 2
FOLD = 3
F32 = jnp.float32
BF16 = jnp.bfloat16
I32 = jnp.int32
NT = (((1,), (1,)), ((), ()))
NN = (((1,), (0,)), ((), ()))


def iota(shape, axis):
    return lax.broadcasted_iota(I32, shape, axis)


def pick(table, idx):
    return jnp.take_along_axis(table, idx, axis=1, mode="promise_in_bounds")


def row_to(value, rows):
    return jnp.broadcast_to(value, (rows, value.shape[1]))


def table_lookup(table_ref, ids, rows, init):
    out = jnp.full(ids.shape, init, F32)
    for r in range(rows):
        hit = pick(row_to(table_ref[r : r + 1, :], ids.shape[0]), ids & (LANES - 1))
        out = jnp.where((ids >> 7) == r, hit, out)
    return out


def tile_kernel(
    dims, mix_ref, band_ref, raw_ref, mag_ref, lists_ref, colors_ref, out_ref, tab_ref, pad_ref, sq_ref, wf_ref, x_ref, colf_ref
):
    bands, obs, stars, blocks, entries, fields, blk_rows = dims
    lane = iota((SUBS, LANES), 1)
    pad_ref[...] = jnp.full((SUBS, LANES), fields, I32)
    pad_ref[:, :entries] = lists_ref[...]
    ids = pad_ref[...]
    live = ids < fields
    safe = jnp.where(live, ids, 0)
    colf_ref[...] = colors_ref[...].astype(F32)
    color = table_lookup(colf_ref, safe, fields // LANES, 0.0).astype(I32)
    key = jnp.where(live, color * entries + lane, COLORS * entries)
    rank = jnp.zeros((SUBS, LANES), I32)
    for e in range(entries):
        rank = rank + jnp.where(key[:, e : e + 1] < key, 1, 0)
    live_f = jnp.where(live, 1.0, 0.0)
    dead = entries - jnp.sum(live_f, axis=1, keepdims=True).astype(I32)
    pos = jnp.where(live, rank + ((dead * color) >> (COLORS.bit_length() - 1)), 4 * LANES)
    inv = jnp.full((SUBS, LANES), -1, I32)
    for e in range(entries):
        inv = jnp.where(pos[:, e : e + 1] == lane, e, inv)
    used = inv >= 0
    inv_safe = jnp.where(used, inv, 0)
    fpos = jnp.where(used, pick(ids, inv_safe).astype(F32), -1.0)
    cpos = jnp.where(used, pick(color, inv_safe).astype(F32), float(COLORS))
    pos_live = jnp.where(live, pos, 0)
    tab_ref[...] = ((pos_live >> 1) & 1) * HALF + (pos_live >> 2) * (2 * bands) + (pos_live & 1) * bands

    sq_ref[...] = jnp.zeros((LANES, LANES), F32)
    sq_ref[0:SUBS, :] = inv.astype(F32)
    inv_t = sq_ref[...].T
    mine = band_ref[0]
    lanes_sq = iota((entries, LANES), 1)
    t0_cols = jnp.zeros((entries, LANES), F32)
    wt_cols = jnp.zeros((entries, LANES), F32)
    for blk in range(blocks):
        lo, hi = blk * blk_rows, (blk + 1) * blk_rows
        inv_col = jnp.broadcast_to(inv_t[0:entries, blk : blk + 1], (entries, blk_rows))
        pred = jnp.zeros((1, blk_rows), F32)
        for b in range(bands):
            w = raw_ref[b, 0:obs, lo:hi]
            slot = raw_ref[b, obs : 2 * obs, lo:hi]
            acc = jnp.zeros((entries, blk_rows), F32)
            for k in range(obs):
                acc = acc + jnp.where(slot[k : k + 1] == inv_col, w[k : k + 1], 0.0)
            scale = mix_ref[b] / jnp.sum(w, axis=0, keepdims=True)
            wf_ref[b * entries : (b + 1) * entries, :] = acc
            x_ref[b * entries : (b + 1) * entries, :] = acc * scale
            pieces = blk_rows // LANES
            means = raw_ref[b, blk * pieces : (blk + 1) * pieces, stars : stars + LANES]
            pred = pred + mix_ref[b] * jnp.concatenate([means[i : i + 1] for i in range(pieces)], axis=1)
        own = wf_ref[pl.ds(mine * entries, entries), :]
        gram = lax.dot_general(own, x_ref[...], NT, precision=lax.Precision.HIGHEST, preferred_element_type=F32)
        out_ref[pl.ds(blk, entries, stride=SUBS), :] = gram
        w = raw_ref[mine, 0:obs, lo:hi]
        slot = raw_ref[mine, obs : 2 * obs, lo:hi]
        value = w * (mag_ref[:, lo:hi] - pred)
        acc = jnp.zeros((entries, blk_rows), F32)
        for k in range(obs):
            acc = acc + jnp.where(slot[k : k + 1] == inv_col, value[k : k + 1], 0.0)
        t0_cols = jnp.where(lanes_sq == blk, jnp.sum(acc, axis=1, keepdims=True), t0_cols)
        wt_cols = jnp.where(lanes_sq == blk, jnp.sum(own, axis=1, keepdims=True), wt_cols)
    sq_ref[...] = jnp.zeros((LANES, LANES), F32)
    sq_ref[0:entries, :] = t0_cols
    sq_ref[entries : 2 * entries, :] = wt_cols
    flipped = sq_ref[...].T[0:SUBS]
    extra = jnp.where(lane < 3 * entries, pltpu.roll(fpos, 2 * entries, 1), pltpu.roll(cpos, 3 * entries, 1))
    out_ref[entries * SUBS : (entries + 1) * SUBS, :] = jnp.where(lane < 2 * entries, flipped, extra)


def split3(value):
    hi = value.astype(BF16).astype(F32)
    rest = value - hi
    mid = rest.astype(BF16).astype(F32)
    return hi, mid, rest - mid


def sweep_kernel(
    dims, mix_ref, place_ref, all_ref, raw_ref, mag_ref, tab_ref, owner_ref,
    zp_ref, means_ref, misfit_ref,
    et_ref, v_ref, den_ref, fld_ref, col_ref, g_ref, s_ref, z_ref, dz_ref, zs_ref,
    sq_ref, lim_ref, fc_ref, fr_ref, tv_ref, ze_ref, rk_ref, big_ref,
):
    tiles, bands, obs, stars, blocks, entries, fields, blk_rows, owned = dims
    groups = entries // 4
    pair = 2 * bands
    vrows = groups * pair
    rows_dev = (entries + 1) * SUBS
    lane8 = iota((SUBS, LANES), 1)
    low8 = lane8 < HALF
    my_tile, mine = place_ref[0], place_ref[1]

    for b in range(bands):
        sq_ref[...] = jnp.zeros((LANES, LANES), F32)
        for t in range(tiles):
            sq_ref[t * SUBS : (t + 1) * SUBS, :] = all_ref[t * bands + b, entries * SUBS : rows_dev, :]
        et_ref[...] = sq_ref[...].T
        for p in range(2):
            for q, dest in enumerate((v_ref, den_ref, fld_ref, col_ref)):
                first = et_ref[pl.ds(q * entries + p, groups, stride=4), :]
                second = et_ref[pl.ds(q * entries + 2 + p, groups, stride=4), :]
                dest[pl.ds(p * bands + b, groups, stride=pair), :] = jnp.where(low8, first, pltpu.roll(second, HALF, 1))

    def turn(k, carry):
        for p in range(2):
            for b in range(bands):
                parts = []
                for half in range(2):
                    start = pl.multiple_of((4 * k + 2 * half + p) * SUBS, SUBS)
                    for t in range(tiles):
                        parts.append(all_ref[t * bands + b, pl.ds(start, SUBS), :])
                flipped = jnp.concatenate(parts, axis=0).T
                for b2 in range(bands):
                    g_ref[pl.ds(b2 * vrows + k * pair + p * bands + b, entries, stride=bands * vrows), :] = flipped[
                        b2 * entries : (b2 + 1) * entries
                    ]
        return carry

    lax.fori_loop(0, groups, turn, 0)

    srows = 2 * groups
    fld2 = fld_ref[pl.ds(0, srows, stride=bands), :]
    col2 = col_ref[pl.ds(0, srows, stride=bands), :]
    row2 = iota((srows, LANES), 0)
    position = 4 * (row2 >> 1) + 2 * jnp.where(iota((srows, LANES), 1) < HALF, 0, 1) + (row2 & 1)
    most = jnp.zeros((1, LANES), F32)
    for c in range(COLORS):
        hit = col2 == float(c)
        lim_ref[0, c] = jnp.min(jnp.where(hit, position, entries))
        lim_ref[1, c] = jnp.max(jnp.where(hit, position + 1, 0))
        count = jnp.sum(jnp.where(hit, 1.0, 0.0), axis=0, keepdims=True)
        most = jnp.maximum(most, count + pltpu.roll(count, HALF, 1))
    fits = jnp.max(most) <= 4.0 * FOLD

    def build(c, carry):
        hit = col2 == c.astype(F32)
        chosen = jnp.where(hit, fld2, -1.0)
        folded = []
        for m in range(FOLD):
            for p in range(2):
                best = jnp.full((1, LANES), -1.0, F32)
                for k in range(m, groups, FOLD):
                    best = jnp.maximum(best, chosen[2 * k + p : 2 * k + p + 1])
                folded.append(best)
        sq_ref[0 : 2 * FOLD, :] = jnp.concatenate(folded, axis=0)
        columns = sq_ref[...].T
        for i in range(2 * FOLD):
            col = jnp.broadcast_to(columns[:, i : i + 1], (LANES, LANES))
            for j in range(2 * FOLD):
                row = jnp.where(folded[j] < 0.0, -2.0, folded[j])
                tile = jnp.where(col == row, 1.0, 0.0).astype(BF16)
                m, p, n, r = i // 2, i % 2, j // 2, j % 2
                s_ref[c * FOLD * FOLD + m * FOLD + n, p * LANES : (p + 1) * LANES, r * LANES : (r + 1) * LANES] = tile
        return carry

    lax.fori_loop(0, COLORS, build, 0)

    def spread_rows(value):
        flat = jnp.concatenate([value[0:bands], value[bands:pair]], axis=1)
        hi, mid, lo = split3(flat)
        return jnp.concatenate([hi, mid, lo, jnp.zeros_like(hi)], axis=0).astype(BF16)

    def pack_rows(total):
        flat = total[0:bands] + (total[bands : 2 * bands] + total[2 * bands : 3 * bands])
        return jnp.concatenate([flat[:, :LANES], flat[:, LANES:]], axis=0)

    def same_field(c, src):
        cf = c.astype(F32)

        @pl.when(fits)
        def fast():
            lhs = []
            for m in range(FOLD):
                fold = jnp.zeros((pair, LANES), F32)
                for k in range(m, groups, FOLD):
                    rows = slice(k * pair, (k + 1) * pair)
                    fold = fold + jnp.where(col_ref[rows] == cf, src[rows], 0.0)
                lhs.append(spread_rows(fold))
            for n in range(FOLD):
                total = jnp.zeros((4 * bands, 2 * LANES), F32)
                for m in range(FOLD):
                    total = total + lax.dot_general(
                        lhs[m], s_ref[c * FOLD * FOLD + m * FOLD + n], NN, preferred_element_type=F32
                    )
                packed = pack_rows(total)
                for k in range(n, groups, FOLD):
                    tv_ref[k * pair : (k + 1) * pair, :] = packed

        @pl.when(jnp.logical_not(fits))
        def general():
            chosen = jnp.where(col2 == cf, fld2, -1.0)
            sq_ref[...] = jnp.full((LANES, LANES), -1.0, F32)
            sq_ref[0:srows, :] = chosen
            columns = sq_ref[...].T
            for i in range(srows):
                fc_ref[i] = jnp.broadcast_to(columns[:, i : i + 1], (LANES, LANES))
                fr_ref[i] = row_to(jnp.where(chosen[i : i + 1] < 0.0, -2.0, chosen[i : i + 1]), SUBS)
            for m in range(groups):
                rows = slice(m * pair, (m + 1) * pair)
                big_ref[m] = spread_rows(jnp.where(col_ref[rows] == cf, src[rows], 0.0)).astype(F32)

            def outer(n, carry):
                def inner(m, total):
                    parts = []
                    for r in range(2):
                        row = fr_ref[2 * n + r][0:1]
                        upper = jnp.where(fc_ref[2 * m] == row, 1.0, 0.0)
                        lower = jnp.where(fc_ref[2 * m + 1] == row, 1.0, 0.0)
                        lhs = big_ref[m].astype(BF16)
                        parts.append(
                            lax.dot_general(lhs[:, :LANES], upper.astype(BF16), NN, preferred_element_type=F32)
                            + lax.dot_general(lhs[:, LANES:], lower.astype(BF16), NN, preferred_element_type=F32)
                        )
                    return total + jnp.concatenate(parts, axis=1)

                total = lax.fori_loop(0, groups, inner, jnp.zeros((4 * bands, 2 * LANES), F32))
                tv_ref[pl.ds(pl.multiple_of(n * pair, pair), pair), :] = pack_rows(total)
                return carry

            lax.fori_loop(0, groups, outer, 0)

    z_ref[...] = jnp.full((vrows, LANES), PRIOR_WEIGHT, F32)

    def denominator(c, carry):
        same_field(c, den_ref)
        z_ref[...] = z_ref[...] + jnp.where(col_ref[...] == c.astype(F32), tv_ref[...], 0.0)
        return carry

    lax.fori_loop(0, COLORS, denominator, 0)
    den_ref[...] = 1.0 / z_ref[...]
    z_ref[...] = jnp.zeros((vrows, LANES), F32)

    def step(n, carry):
        c = n & (COLORS - 1)
        cf = c.astype(F32)
        same_field(c, v_ref)
        for k in range(groups):
            rows = slice(k * pair, (k + 1) * pair)
            old = z_ref[rows]
            new = jnp.where(col_ref[rows] == cf, tv_ref[rows] * den_ref[rows], old)
            z_ref[rows] = new
            diff = new - old
            turned = pltpu.roll(diff, HALF, 1)
            dz_ref[2 * k * pair : (2 * k + 1) * pair, :] = jnp.where(low8, diff, turned)
            dz_ref[(2 * k + 1) * pair : (2 * k + 2) * pair, :] = jnp.where(low8, turned, diff)

        def apply(p, accs):
            accs = list(accs)
            for b2 in range(bands):
                j = p * bands + b2
                row = row_to(dz_ref[pl.ds(j, 1), :], pair)
                for k in range(groups):
                    base = pl.multiple_of(j * vrows + k * pair, pair)
                    accs[k] = accs[k] + g_ref[pl.ds(base, pair), :] * row
            return tuple(accs)

        start = tuple(v_ref[k * pair : (k + 1) * pair] for k in range(groups))
        done = lax.fori_loop(lim_ref[0, c], lim_ref[1, c], apply, start)
        for k in range(groups):
            v_ref[k * pair : (k + 1) * pair, :] = done[k]

        @pl.when(c == COLORS - 1)
        def keep():
            zs_ref[n >> (COLORS.bit_length() - 1)] = z_ref[...]

        return carry

    lax.fori_loop(0, SWEEPS * COLORS, step, 0)

    tab = tab_ref[...]
    for sweep in range(SWEEPS):
        sq_ref[...] = jnp.zeros((LANES, LANES), F32)
        sq_ref[0:vrows, :] = zs_ref[sweep]
        et_ref[...] = sq_ref[...].T
        first = et_ref[pl.ds(pl.multiple_of(my_tile * SUBS, SUBS), SUBS), :]
        second = et_ref[pl.ds(pl.multiple_of(HALF + my_tile * SUBS, SUBS), SUBS), :]
        table = jnp.where(low8, first, pltpu.roll(second, HALF, 1))
        for b in range(bands):
            ze_ref[sweep * bands + b] = pick(table, tab + b)

    squares = [jnp.zeros((obs, LANES), F32) for _ in range(SWEEPS)]
    for chunk in range(stars // LANES):
        at = slice(chunk * LANES, (chunk + 1) * LANES)
        blk = chunk * LANES // blk_rows
        pred = [jnp.zeros((1, LANES), F32) for _ in range(SWEEPS)]
        own_mean = jnp.zeros((1, LANES), F32)
        for b in range(bands):
            w = raw_ref[b, 0:obs, at]
            slot = raw_ref[b, obs : 2 * obs, at].astype(I32)
            inverse = 1.0 / jnp.sum(w, axis=0, keepdims=True)
            base = raw_ref[b, chunk : chunk + 1, stars : stars + LANES]
            for sweep in range(SWEEPS):
                seen = pick(row_to(ze_ref[sweep * bands + b, blk : blk + 1, :], obs), slot)
                mean = base - jnp.sum(w * seen, axis=0, keepdims=True) * inverse
                pred[sweep] = pred[sweep] + mix_ref[b] * mean
                if sweep == SWEEPS - 1:
                    own_mean = jnp.where(mine == b, mean, own_mean)
        means_ref[0:1, at] = own_mean
        w = raw_ref[mine, 0:obs, at]
        slot = raw_ref[mine, obs : 2 * obs, at].astype(I32)
        mag = mag_ref[:, at]
        for sweep in range(SWEEPS):
            seen = pick(row_to(ze_ref[sweep * bands + mine, blk : blk + 1, :], obs), slot)
            gap = mag - pred[sweep] - seen
            squares[sweep] = squares[sweep] + w * gap * gap
    result = jnp.zeros((SUBS, LANES), F32)
    for sweep in range(SWEEPS):
        result = jnp.where(lane8 == sweep, jnp.sum(squares[sweep]), result)
    misfit_ref[...] = result

    frows = fields // LANES
    own = jnp.where(owner_ref[...] == my_tile, 1.0, 0.0)
    upto = jnp.where(iota((LANES, LANES), 0) <= iota((LANES, LANES), 1), 1.0, 0.0).astype(BF16)
    inside = lax.dot_general(own.astype(BF16), upto, NN, preferred_element_type=F32)
    sums = jnp.broadcast_to(jnp.sum(own, axis=1, keepdims=True), (frows, LANES))
    before = jnp.where(iota((frows, frows), 1) < iota((frows, frows), 0), 1.0, 0.0).astype(BF16)
    ahead = lax.dot_general(before, sums.astype(BF16), NN, preferred_element_type=F32)
    rk_ref[...] = jnp.where(own > 0.0, inside + ahead - 1.0, -1.0)
    ids = jnp.where(fld2 < 0.0, 0.0, fld2).astype(I32)
    ranks = jnp.where(fld2 < 0.0, -1.0, table_lookup(rk_ref, ids, frows, -1.0))
    sq_ref[...] = jnp.full((LANES, LANES), -1.0, F32)
    sq_ref[0:srows, :] = ranks
    columns = sq_ref[...].T
    hi, mid, lo = split3(z_ref[pl.ds(mine, srows, stride=bands), :])
    places = iota((LANES, owned), 1).astype(F32)
    ones = jnp.ones((1, LANES), F32)
    total = jnp.zeros((SUBS, owned), F32)
    for r in range(srows):
        one_hot = jnp.where(jnp.broadcast_to(columns[:, r : r + 1], (LANES, owned)) == places, 1.0, 0.0)
        lhs = jnp.concatenate([hi[r : r + 1], mid[r : r + 1], lo[r : r + 1], ones, jnp.zeros((4, LANES), F32)], axis=0)
        total = total + lax.dot_general(lhs.astype(BF16), one_hot.astype(BF16), NN, preferred_element_type=F32)
    zp_ref[...] = (total[0:1] + (total[1:2] + total[2:3])) / jnp.maximum(total[3:4], 1.0)


def vmem():
    return pl.BlockSpec(memory_space=pltpu.VMEM)


def smem():
    return pl.BlockSpec(memory_space=pltpu.SMEM)


def replicate(payload):
    return lax.all_gather(payload, ("sky", "band"), axis=0)


def sky_sum(value):
    return lax.psum(value, "sky")


def local_body(magnitudes, weights, slots, block_fields, owner, colors, color_terms):
    bands = color_terms.shape[0]
    tiles = lax.axis_size("sky")
    my_tile = lax.axis_index("sky")
    my_band = lax.axis_index("band")
    _, obs, stars = magnitudes.shape
    blocks, entries = block_fields.shape
    fields = owner.shape[0]
    blk_rows = stars // blocks
    owned = fields // tiles
    mags, wts, slt = magnitudes[0], weights[0], slots[0]
    base = jnp.sum(wts * mags, axis=0) / jnp.sum(wts, axis=0)
    mixing = jnp.eye(bands, dtype=F32) + color_terms - jnp.diag(jnp.sum(color_terms, axis=1))
    mix_row = lax.dynamic_index_in_dim(mixing, my_band, 0, keepdims=False)
    left = jnp.concatenate([wts, slt.astype(F32)], axis=0)
    raw = lax.all_gather(jnp.concatenate([left, base.reshape(2 * obs, LANES)], axis=1), "band", axis=0)
    place = jnp.stack([my_tile, my_band]).astype(I32)

    rows_dev = (entries + 1) * SUBS
    payload, tab = pl.pallas_call(
        functools.partial(tile_kernel, (bands, obs, stars, blocks, entries, fields, blk_rows)),
        name="tile",
        out_shape=(jax.ShapeDtypeStruct((rows_dev, LANES), F32), jax.ShapeDtypeStruct((SUBS, LANES), I32)),
        in_specs=[smem(), smem(), vmem(), vmem(), vmem(), vmem()],
        out_specs=(vmem(), vmem()),
        scratch_shapes=[
            pltpu.VMEM((SUBS, LANES), I32),
            pltpu.VMEM((LANES, LANES), F32),
            pltpu.VMEM((bands * entries, blk_rows), F32),
            pltpu.VMEM((bands * entries, blk_rows), F32),
            pltpu.VMEM((fields // LANES, LANES), F32),
        ],
    )(mix_row, place[1:], raw, mags, block_fields, colors.reshape(-1, LANES))

    everything = replicate(payload)

    groups = entries // 4
    pair = 2 * bands
    vrows = groups * pair
    zp, means, partial = pl.pallas_call(
        functools.partial(sweep_kernel, (tiles, bands, obs, stars, blocks, entries, fields, blk_rows, owned)),
        name="sweeps",
        out_shape=(
            jax.ShapeDtypeStruct((1, owned), F32),
            jax.ShapeDtypeStruct((1, stars), F32),
            jax.ShapeDtypeStruct((SUBS, LANES), F32),
        ),
        in_specs=[smem(), smem()] + [vmem()] * 5,
        out_specs=(vmem(), vmem(), vmem()),
        scratch_shapes=[
            pltpu.VMEM((LANES, LANES), F32),
            pltpu.VMEM((vrows, LANES), F32),
            pltpu.VMEM((vrows, LANES), F32),
            pltpu.VMEM((vrows, LANES), F32),
            pltpu.VMEM((vrows, LANES), F32),
            pltpu.VMEM((bands * entries * vrows, LANES), F32),
            pltpu.VMEM((COLORS * FOLD * FOLD, 2 * LANES, 2 * LANES), BF16),
            pltpu.VMEM((vrows, LANES), F32),
            pltpu.VMEM((bands * entries, LANES), F32),
            pltpu.VMEM((SWEEPS, vrows, LANES), F32),
            pltpu.VMEM((LANES, LANES), F32),
            pltpu.SMEM((2, COLORS), I32),
            pltpu.VMEM((2 * groups, LANES, LANES), F32),
            pltpu.VMEM((2 * groups, SUBS, LANES), F32),
            pltpu.VMEM((vrows, LANES), F32),
            pltpu.VMEM((SWEEPS * bands, SUBS, LANES), F32),
            pltpu.VMEM((fields // LANES, LANES), F32),
            pltpu.VMEM((groups, 4 * bands, 2 * LANES), F32),
        ],
        compiler_params=pltpu.CompilerParams(vmem_limit_bytes=56 * 1024 * 1024),
    )(mix_row, place, everything, raw, mags, tab, owner.reshape(-1, LANES))

    misfit = sky_sum(partial[0, :SWEEPS]) / (obs * stars * tiles)
    return zp, means, misfit[:, None]


def fits_local(mesh, blocks_all, entries, stars, obs, bands, fields):
    tiles = mesh.shape["sky"]
    blocks = blocks_all // tiles
    return (
        2 * blocks_all == LANES
        and blocks == SUBS
        and bands * entries == LANES
        and obs == SUBS
        and 2 * bands == SUBS
        and mesh.shape["band"] == bands
        and stars // tiles == 2 * obs * LANES
        and (stars // blocks_all) % LANES == 0
        and fields % (tiles * LANES) == 0
    )


def from_behind(value, axis, steps):
    count = lax.axis_size(axis)
    pairs = [(source, (source + steps) % count) for source in range(count)]
    return lax.ppermute(value, axis, pairs)


def wide_body(magnitudes, weights, slots, block_fields, owner, colors, color_terms):
    band_count = color_terms.shape[0]
    tiles = lax.axis_size("sky")
    my_tile = lax.axis_index("sky")
    my_band = lax.axis_index("band")
    band_mags, band_wts, band_slots = (magnitudes, weights, slots)
    own_row = 0
    band_rows, obs_count, star_count = band_mags.shape
    block_count, list_len = block_fields.shape
    block_rows = star_count // block_count
    fields = owner.shape[0]
    slot_grid = band_slots.reshape(band_rows, obs_count, block_count, block_rows)
    entries = jnp.arange(list_len, dtype=jnp.int32)
    star_weight = jnp.sum(band_wts, axis=1)
    mixing = (
        jnp.eye(band_count, dtype=jnp.float32)
        + color_terms
        - jnp.diag(jnp.sum(color_terms, axis=1))
    )
    owner_order = jnp.argsort(owner, stable=True)
    owned = fields // tiles

    def slot_sums(values):
        grid = values.reshape(band_rows, obs_count, block_count, block_rows)
        hits = slot_grid[..., None] == entries
        return jnp.sum(jnp.where(hits, grid[..., None], 0.0), axis=(1, 3))

    def spread(list_vals):
        hits = slot_grid[..., None] == entries
        picked = jnp.sum(jnp.where(hits, list_vals[:, None, :, None, :], 0.0), axis=4)
        return picked.reshape(band_rows, obs_count, star_count)

    def predict(zp_obs):
        star_means = jnp.sum(band_wts * (band_mags - zp_obs), axis=1) / star_weight
        all_means = lax.all_gather(star_means, "band", axis=0, tiled=True)
        mix_row = lax.dynamic_index_in_dim(mixing, my_band, 0, keepdims=True)
        predicted = jnp.dot(mix_row, all_means, precision=lax.Precision.HIGHEST)
        return (star_means, predicted)

    positions = jnp.argsort(owner_order, stable=True)
    rank_in = positions - owner * owned
    live = block_fields < fields
    safe_ids = jnp.minimum(block_fields, fields - 1)
    relative = jnp.mod(jnp.take(owner, safe_ids) - my_tile + 1, tiles)
    list_ids = jnp.where(live, relative * owned + jnp.take(rank_in, safe_ids), 3 * owned)
    segments = 3 * owned
    nearby_idx = jnp.mod(my_tile + jnp.arange(3, dtype=jnp.int32) - 1, tiles)
    near_fields = jnp.take(owner_order.reshape(tiles, owned), nearby_idx, axis=0)
    zp_colors = jnp.take(colors, near_fields)[None]
    zero_pts = jnp.zeros((band_rows, 3, owned), jnp.float32)

    def flatten(table):
        return table.reshape(band_rows, 3 * owned)

    def combine(partial_flat):
        partial_sums = partial_flat.reshape(band_rows, 3, owned)
        from_left = from_behind(partial_sums[:, 1:3], "sky", 1)
        from_right = from_behind(partial_sums[:, 0:2], "sky", -1)
        far_left = from_behind(partial_sums[:, 2], "sky", 2)
        far_right = from_behind(partial_sums[:, 0], "sky", -2)
        below = far_left + from_left[:, 0] + partial_sums[:, 0]
        middle = from_left[:, 1] + partial_sums[:, 1] + from_right[:, 0]
        above = partial_sums[:, 2] + from_right[:, 1] + far_right
        return jnp.stack([below, middle, above], axis=1)

    def lookup(table):
        padded = jnp.concatenate([flatten(table), jnp.zeros((band_rows, 1), jnp.float32)], axis=1)
        return spread(jnp.take(padded, list_ids, axis=1))

    def segment_band(per_band):
        return jax.ops.segment_sum(
            per_band.reshape(-1), list_ids.reshape(-1), num_segments=segments + 1
        )[:segments]

    def totals(values):
        per_slot = slot_sums(values)
        return combine(jax.vmap(segment_band)(per_slot))

    denominators = totals(band_wts) + PRIOR_WEIGHT

    def squared_misfit(residual, zp_obs):
        per_band = jnp.sum(band_wts * (residual - zp_obs) ** 2, axis=(1, 2))
        return lax.dynamic_index_in_dim(per_band, own_row, 0, keepdims=False)

    def advance(table, color_no):
        zp_obs = lookup(table)
        star_means, predicted = predict(zp_obs)
        residual = band_mags - predicted[:, None, :]
        updated = totals(band_wts * residual) / denominators
        local_value = squared_misfit(residual, zp_obs)
        return (jnp.where(zp_colors == color_no, updated, table), local_value)

    def later_colors(color_no, table):
        return advance(table, color_no)[0]

    def record(local_value):
        return lax.psum(local_value, "sky")

    recorded = []
    for sweep_no in range(SWEEPS):
        zero_pts, local_value = advance(zero_pts, 0)
        if sweep_no > 0:
            recorded.append(record(local_value))
        zero_pts = lax.fori_loop(1, COLORS, later_colors, zero_pts)
    zp_obs = lookup(zero_pts)
    star_means, predicted = predict(zp_obs)
    residual = band_mags - predicted[:, None, :]
    recorded.append(record(squared_misfit(residual, zp_obs)))
    stacked = jnp.stack(recorded)
    misfit = stacked / (obs_count * star_count * tiles)
    own_zp = lax.dynamic_index_in_dim(zero_pts[:, 1], own_row, 0, keepdims=True)
    own_means = lax.dynamic_index_in_dim(star_means, own_row, 0, keepdims=True)
    return (own_zp, own_means, misfit[:, None])


def solution(mesh):
    in_specs = (
        P("band", None, "sky"),
        P("band", None, "sky"),
        P("band", None, "sky"),
        P("sky", None),
        P(),
        P(),
        P(),
    )
    out_specs = (P("band", "sky"), P("band", "sky"), P(None, "band"))

    def call(magnitudes, weights, slots, block_fields, owner, colors, color_terms):
        bands, obs, stars = magnitudes.shape
        blocks_all, entries = block_fields.shape
        local = fits_local(mesh, blocks_all, entries, stars, obs, bands, owner.shape[0])
        body = local_body if local else wide_body
        run = jax.shard_map(body, mesh=mesh, in_specs=in_specs, out_specs=out_specs, check_vma=False)
        return run(magnitudes, weights, slots, block_fields, owner, colors, color_terms)

    return call
```

```python
import functools

import jax
import jax.numpy as jnp
from jax import lax
from jax.experimental import pallas as pl
from jax.experimental.pallas import tpu as pltpu
from jax.sharding import PartitionSpec as P

COLORS = 8
SWEEPS = 4


PRIOR_WEIGHT = 1.0
LANES = 128
SUBS = 8
HALF = LANES // 2
FOLD = 3
F32 = jnp.float32
BF16 = jnp.bfloat16
I32 = jnp.int32
NT = (((1,), (1,)), ((), ()))
NN = (((1,), (0,)), ((), ()))


def iota(shape, axis):
    return lax.broadcasted_iota(I32, shape, axis)


def pick(table, idx):
    return jnp.take_along_axis(table, idx, axis=1, mode="promise_in_bounds")


def row_to(value, rows):
    return jnp.broadcast_to(value, (rows, value.shape[1]))


def table_lookup(table_ref, ids, rows, init):
    out = jnp.full(ids.shape, init, F32)
    for r in range(rows):
        hit = pick(row_to(table_ref[r : r + 1, :], ids.shape[0]), ids & (LANES - 1))
        out = jnp.where((ids >> 7) == r, hit, out)
    return out


def mixing_row(terms_ref, mine, bands):
    total = terms_ref[mine, 0]
    for b in range(1, bands):
        total = total + terms_ref[mine, b]
    return [terms_ref[mine, b] + jnp.where(mine == b, 1.0 - total, 0.0) for b in range(bands)]


def pack_kernel(mag_ref, wt_ref, slot_ref, out_ref):
    obs, stars = mag_ref.shape
    w = wt_ref[...]
    out_ref[0:obs, 0:stars] = w
    out_ref[obs : 2 * obs, 0:stars] = slot_ref[...].astype(F32)
    base = jnp.sum(w * mag_ref[...], axis=0, keepdims=True) / jnp.sum(w, axis=0, keepdims=True)
    for i in range(stars // LANES):
        out_ref[i : i + 1, stars : stars + LANES] = base[:, i * LANES : (i + 1) * LANES]


def tile_kernel(
    dims, terms_ref, raw_ref, mag_ref, lists_ref, colors_ref, out_ref, tab_ref, pad_ref, sq_ref, wf_ref, x_ref, colf_ref
):
    bands, obs, stars, blocks, entries, fields, blk_rows = dims
    lane = iota((SUBS, LANES), 1)
    pad_ref[...] = jnp.full((SUBS, LANES), fields, I32)
    pad_ref[:, :entries] = lists_ref[...]
    ids = pad_ref[...]
    live = ids < fields
    safe = jnp.where(live, ids, 0)
    colf_ref[...] = colors_ref[...].astype(F32)
    color = table_lookup(colf_ref, safe, fields // LANES, 0.0).astype(I32)
    key = jnp.where(live, color * entries + lane, COLORS * entries)
    rank = jnp.zeros((SUBS, LANES), I32)
    for e in range(entries):
        rank = rank + jnp.where(key[:, e : e + 1] < key, 1, 0)
    live_f = jnp.where(live, 1.0, 0.0)
    dead = entries - jnp.sum(live_f, axis=1, keepdims=True).astype(I32)
    pos = jnp.where(live, rank + ((dead * color) >> (COLORS.bit_length() - 1)), 4 * LANES)
    inv = jnp.full((SUBS, LANES), -1, I32)
    for e in range(entries):
        inv = jnp.where(pos[:, e : e + 1] == lane, e, inv)
    used = inv >= 0
    inv_safe = jnp.where(used, inv, 0)
    fpos = jnp.where(used, pick(ids, inv_safe).astype(F32), -1.0)
    cpos = jnp.where(used, pick(color, inv_safe).astype(F32), float(COLORS))
    pos_live = jnp.where(live, pos, 0)
    tab_ref[...] = ((pos_live >> 1) & 1) * HALF + (pos_live >> 2) * (2 * bands) + (pos_live & 1) * bands

    sq_ref[...] = jnp.zeros((LANES, LANES), F32)
    sq_ref[0:SUBS, :] = inv.astype(F32)
    inv_t = sq_ref[...].T
    mine = lax.axis_index("band")
    mix_ref = mixing_row(terms_ref, mine, bands)
    lanes_sq = iota((entries, LANES), 1)
    t0_cols = jnp.zeros((entries, LANES), F32)
    wt_cols = jnp.zeros((entries, LANES), F32)
    for blk in range(blocks):
        lo, hi = blk * blk_rows, (blk + 1) * blk_rows
        inv_col = jnp.broadcast_to(inv_t[0:entries, blk : blk + 1], (entries, blk_rows))
        pred = jnp.zeros((1, blk_rows), F32)
        for b in range(bands):
            w = raw_ref[b, 0:obs, lo:hi]
            slot = raw_ref[b, obs : 2 * obs, lo:hi]
            acc = jnp.zeros((entries, blk_rows), F32)
            for k in range(obs):
                acc = acc + jnp.where(slot[k : k + 1] == inv_col, w[k : k + 1], 0.0)
            scale = mix_ref[b] / jnp.sum(w, axis=0, keepdims=True)
            wf_ref[b * entries : (b + 1) * entries, :] = acc
            x_ref[b * entries : (b + 1) * entries, :] = acc * scale
            pieces = blk_rows // LANES
            means = raw_ref[b, blk * pieces : (blk + 1) * pieces, stars : stars + LANES]
            pred = pred + mix_ref[b] * jnp.concatenate([means[i : i + 1] for i in range(pieces)], axis=1)
        own = wf_ref[pl.ds(mine * entries, entries), :]
        gram = lax.dot_general(own, x_ref[...], NT, precision=lax.Precision.HIGHEST, preferred_element_type=F32)
        out_ref[pl.ds(blk, entries, stride=SUBS), :] = gram
        w = raw_ref[mine, 0:obs, lo:hi]
        slot = raw_ref[mine, obs : 2 * obs, lo:hi]
        value = w * (mag_ref[:, lo:hi] - pred)
        acc = jnp.zeros((entries, blk_rows), F32)
        for k in range(obs):
            acc = acc + jnp.where(slot[k : k + 1] == inv_col, value[k : k + 1], 0.0)
        t0_cols = jnp.where(lanes_sq == blk, jnp.sum(acc, axis=1, keepdims=True), t0_cols)
        wt_cols = jnp.where(lanes_sq == blk, jnp.sum(own, axis=1, keepdims=True), wt_cols)
    sq_ref[...] = jnp.zeros((LANES, LANES), F32)
    sq_ref[0:entries, :] = t0_cols
    sq_ref[entries : 2 * entries, :] = wt_cols
    flipped = sq_ref[...].T[0:SUBS]
    extra = jnp.where(lane < 3 * entries, pltpu.roll(fpos, 2 * entries, 1), pltpu.roll(cpos, 3 * entries, 1))
    out_ref[entries * SUBS : (entries + 1) * SUBS, :] = jnp.where(lane < 2 * entries, flipped, extra)


def split3(value):
    hi = value.astype(BF16).astype(F32)
    rest = value - hi
    mid = rest.astype(BF16).astype(F32)
    return hi, mid, rest - mid


def sweep_kernel(
    dims, terms_ref, own0_ref, own1_ref, far0_ref, far1_ref, raw_ref, mag_ref, tab_ref, owner_ref,
    zp_ref, means_ref, misfit_ref,
    et_ref, v_ref, den_ref, fld_ref, col_ref, g_ref, s_ref, z_ref, dz_ref, zs_ref,
    sq_ref, lim_ref, fc_ref, fr_ref, tv_ref, ze_ref, rk_ref, big_ref, all_ref, sems,
):
    tiles, bands, obs, stars, blocks, entries, fields, blk_rows, owned = dims
    groups = entries // 4
    pair = 2 * bands
    vrows = groups * pair
    rows_dev = (entries + 1) * SUBS
    lane8 = iota((SUBS, LANES), 1)
    low8 = lane8 < HALF
    my_tile, mine = lax.axis_index("sky"), lax.axis_index("band")
    mix_ref = mixing_row(terms_ref, mine, bands)

    layers = tiles // 2
    my_z, my_y, my_x, my_c = my_tile >> 1, my_tile & 1, mine >> 1, mine & 1
    copies = []
    for core, refs in ((my_c, (own0_ref, own1_ref)), (1 - my_c, (far0_ref, far1_ref))):
        for d2 in range(2):
            for d1 in range(2):
                y = my_y ^ jnp.where(core == 0, d1, d2)
                x = my_x ^ jnp.where(core == 0, d2, d1)
                for shift in range(layers):
                    z = (my_z + layers - shift) % layers
                    device = (z * 2 + y) * bands + x * 2 + core
                    copies.append(
                        pltpu.make_async_copy(
                            refs[d2].at[d1 * layers + shift], all_ref.at[device], sems.at[len(copies)]
                        )
                    )
    for copy in copies:
        copy.start()
    for copy in copies:
        copy.wait()

    for b in range(bands):
        sq_ref[...] = jnp.zeros((LANES, LANES), F32)
        for t in range(tiles):
            sq_ref[t * SUBS : (t + 1) * SUBS, :] = all_ref[t * bands + b, entries * SUBS : rows_dev, :]
        et_ref[...] = sq_ref[...].T
        for p in range(2):
            for q, dest in enumerate((v_ref, den_ref, fld_ref, col_ref)):
                first = et_ref[pl.ds(q * entries + p, groups, stride=4), :]
                second = et_ref[pl.ds(q * entries + 2 + p, groups, stride=4), :]
                dest[pl.ds(p * bands + b, groups, stride=pair), :] = jnp.where(low8, first, pltpu.roll(second, HALF, 1))

    def turn(k, carry):
        for p in range(2):
            for b in range(bands):
                parts = []
                for half in range(2):
                    start = pl.multiple_of((4 * k + 2 * half + p) * SUBS, SUBS)
                    for t in range(tiles):
                        parts.append(all_ref[t * bands + b, pl.ds(start, SUBS), :])
                flipped = jnp.concatenate(parts, axis=0).T
                for b2 in range(bands):
                    g_ref[pl.ds(b2 * vrows + k * pair + p * bands + b, entries, stride=bands * vrows), :] = flipped[
                        b2 * entries : (b2 + 1) * entries
                    ]
        return carry

    lax.fori_loop(0, groups, turn, 0)

    srows = 2 * groups
    fld2 = fld_ref[pl.ds(0, srows, stride=bands), :]
    col2 = col_ref[pl.ds(0, srows, stride=bands), :]
    row2 = iota((srows, LANES), 0)
    position = 4 * (row2 >> 1) + 2 * jnp.where(iota((srows, LANES), 1) < HALF, 0, 1) + (row2 & 1)
    most = jnp.zeros((1, LANES), F32)
    for c in range(COLORS):
        hit = col2 == float(c)
        lim_ref[0, c] = jnp.min(jnp.where(hit, position, entries))
        lim_ref[1, c] = jnp.max(jnp.where(hit, position + 1, 0))
        count = jnp.sum(jnp.where(hit, 1.0, 0.0), axis=0, keepdims=True)
        most = jnp.maximum(most, count + pltpu.roll(count, HALF, 1))
    fits = jnp.max(most) <= 4.0 * FOLD

    def build(c, carry):
        hit = col2 == c.astype(F32)
        chosen = jnp.where(hit, fld2, -1.0)
        folded = []
        for m in range(FOLD):
            for p in range(2):
                best = jnp.full((1, LANES), -1.0, F32)
                for k in range(m, groups, FOLD):
                    best = jnp.maximum(best, chosen[2 * k + p : 2 * k + p + 1])
                folded.append(best)
        sq_ref[0 : 2 * FOLD, :] = jnp.concatenate(folded, axis=0)
        columns = sq_ref[...].T
        for i in range(2 * FOLD):
            col = jnp.broadcast_to(columns[:, i : i + 1], (LANES, LANES))
            for j in range(2 * FOLD):
                row = jnp.where(folded[j] < 0.0, -2.0, folded[j])
                tile = jnp.where(col == row, 1.0, 0.0).astype(BF16)
                m, p, n, r = i // 2, i % 2, j // 2, j % 2
                s_ref[c * FOLD * FOLD + m * FOLD + n, p * LANES : (p + 1) * LANES, r * LANES : (r + 1) * LANES] = tile
        return carry

    lax.fori_loop(0, COLORS, build, 0)

    def spread_rows(value):
        flat = jnp.concatenate([value[0:bands], value[bands:pair]], axis=1)
        hi, mid, lo = split3(flat)
        return jnp.concatenate([hi, mid, lo, jnp.zeros_like(hi)], axis=0).astype(BF16)

    def pack_rows(total):
        flat = total[0:bands] + (total[bands : 2 * bands] + total[2 * bands : 3 * bands])
        return jnp.concatenate([flat[:, :LANES], flat[:, LANES:]], axis=0)

    def same_field(c, src):
        cf = c.astype(F32)

        @pl.when(fits)
        def fast():
            lhs = []
            for m in range(FOLD):
                fold = jnp.zeros((pair, LANES), F32)
                for k in range(m, groups, FOLD):
                    rows = slice(k * pair, (k + 1) * pair)
                    fold = fold + jnp.where(col_ref[rows] == cf, src[rows], 0.0)
                lhs.append(spread_rows(fold))
            for n in range(FOLD):
                total = jnp.zeros((4 * bands, 2 * LANES), F32)
                for m in range(FOLD):
                    total = total + lax.dot_general(
                        lhs[m], s_ref[c * FOLD * FOLD + m * FOLD + n], NN, preferred_element_type=F32
                    )
                packed = pack_rows(total)
                for k in range(n, groups, FOLD):
                    tv_ref[k * pair : (k + 1) * pair, :] = packed

        @pl.when(jnp.logical_not(fits))
        def general():
            chosen = jnp.where(col2 == cf, fld2, -1.0)
            sq_ref[...] = jnp.full((LANES, LANES), -1.0, F32)
            sq_ref[0:srows, :] = chosen
            columns = sq_ref[...].T
            for i in range(srows):
                fc_ref[i] = jnp.broadcast_to(columns[:, i : i + 1], (LANES, LANES))
                fr_ref[i] = row_to(jnp.where(chosen[i : i + 1] < 0.0, -2.0, chosen[i : i + 1]), SUBS)
            for m in range(groups):
                rows = slice(m * pair, (m + 1) * pair)
                big_ref[m] = spread_rows(jnp.where(col_ref[rows] == cf, src[rows], 0.0)).astype(F32)

            def outer(n, carry):
                def inner(m, total):
                    parts = []
                    for r in range(2):
                        row = fr_ref[2 * n + r][0:1]
                        upper = jnp.where(fc_ref[2 * m] == row, 1.0, 0.0)
                        lower = jnp.where(fc_ref[2 * m + 1] == row, 1.0, 0.0)
                        lhs = big_ref[m].astype(BF16)
                        parts.append(
                            lax.dot_general(lhs[:, :LANES], upper.astype(BF16), NN, preferred_element_type=F32)
                            + lax.dot_general(lhs[:, LANES:], lower.astype(BF16), NN, preferred_element_type=F32)
                        )
                    return total + jnp.concatenate(parts, axis=1)

                total = lax.fori_loop(0, groups, inner, jnp.zeros((4 * bands, 2 * LANES), F32))
                tv_ref[pl.ds(pl.multiple_of(n * pair, pair), pair), :] = pack_rows(total)
                return carry

            lax.fori_loop(0, groups, outer, 0)

    z_ref[...] = jnp.full((vrows, LANES), PRIOR_WEIGHT, F32)

    def denominator(c, carry):
        same_field(c, den_ref)
        z_ref[...] = z_ref[...] + jnp.where(col_ref[...] == c.astype(F32), tv_ref[...], 0.0)
        return carry

    lax.fori_loop(0, COLORS, denominator, 0)
    den_ref[...] = 1.0 / z_ref[...]
    z_ref[...] = jnp.zeros((vrows, LANES), F32)

    def step(n, carry):
        c = n & (COLORS - 1)
        cf = c.astype(F32)
        same_field(c, v_ref)
        for k in range(groups):
            rows = slice(k * pair, (k + 1) * pair)
            old = z_ref[rows]
            new = jnp.where(col_ref[rows] == cf, tv_ref[rows] * den_ref[rows], old)
            z_ref[rows] = new
            diff = new - old
            turned = pltpu.roll(diff, HALF, 1)
            dz_ref[2 * k * pair : (2 * k + 1) * pair, :] = jnp.where(low8, diff, turned)
            dz_ref[(2 * k + 1) * pair : (2 * k + 2) * pair, :] = jnp.where(low8, turned, diff)

        def apply(p, accs):
            accs = list(accs)
            for b2 in range(bands):
                j = p * bands + b2
                row = row_to(dz_ref[pl.ds(j, 1), :], pair)
                for k in range(groups):
                    base = pl.multiple_of(j * vrows + k * pair, pair)
                    accs[k] = accs[k] + g_ref[pl.ds(base, pair), :] * row
            return tuple(accs)

        start = tuple(v_ref[k * pair : (k + 1) * pair] for k in range(groups))
        done = lax.fori_loop(lim_ref[0, c], lim_ref[1, c], apply, start)
        for k in range(groups):
            v_ref[k * pair : (k + 1) * pair, :] = done[k]

        @pl.when(c == COLORS - 1)
        def keep():
            zs_ref[n >> (COLORS.bit_length() - 1)] = z_ref[...]

        return carry

    lax.fori_loop(0, SWEEPS * COLORS, step, 0)

    tab = tab_ref[...]
    for sweep in range(SWEEPS):
        sq_ref[...] = jnp.zeros((LANES, LANES), F32)
        sq_ref[0:vrows, :] = zs_ref[sweep]
        et_ref[...] = sq_ref[...].T
        first = et_ref[pl.ds(pl.multiple_of(my_tile * SUBS, SUBS), SUBS), :]
        second = et_ref[pl.ds(pl.multiple_of(HALF + my_tile * SUBS, SUBS), SUBS), :]
        table = jnp.where(low8, first, pltpu.roll(second, HALF, 1))
        for b in range(bands):
            ze_ref[sweep * bands + b] = pick(table, tab + b)

    squares = [jnp.zeros((obs, LANES), F32) for _ in range(SWEEPS)]
    for chunk in range(stars // LANES):
        at = slice(chunk * LANES, (chunk + 1) * LANES)
        blk = chunk * LANES // blk_rows
        pred = [jnp.zeros((1, LANES), F32) for _ in range(SWEEPS)]
        own_mean = jnp.zeros((1, LANES), F32)
        for b in range(bands):
            w = raw_ref[b, 0:obs, at]
            slot = raw_ref[b, obs : 2 * obs, at].astype(I32)
            inverse = 1.0 / jnp.sum(w, axis=0, keepdims=True)
            base = raw_ref[b, chunk : chunk + 1, stars : stars + LANES]
            for sweep in range(SWEEPS):
                seen = pick(row_to(ze_ref[sweep * bands + b, blk : blk + 1, :], obs), slot)
                mean = base - jnp.sum(w * seen, axis=0, keepdims=True) * inverse
                pred[sweep] = pred[sweep] + mix_ref[b] * mean
                if sweep == SWEEPS - 1:
                    own_mean = jnp.where(mine == b, mean, own_mean)
        means_ref[0:1, at] = own_mean
        w = raw_ref[mine, 0:obs, at]
        slot = raw_ref[mine, obs : 2 * obs, at].astype(I32)
        mag = mag_ref[:, at]
        for sweep in range(SWEEPS):
            seen = pick(row_to(ze_ref[sweep * bands + mine, blk : blk + 1, :], obs), slot)
            gap = mag - pred[sweep] - seen
            squares[sweep] = squares[sweep] + w * gap * gap
    result = jnp.zeros((SUBS, LANES), F32)
    for sweep in range(SWEEPS):
        result = jnp.where(lane8 == sweep, jnp.sum(squares[sweep]), result)
    misfit_ref[...] = result

    frows = fields // LANES
    own = jnp.where(owner_ref[...] == my_tile, 1.0, 0.0)
    upto = jnp.where(iota((LANES, LANES), 0) <= iota((LANES, LANES), 1), 1.0, 0.0).astype(BF16)
    inside = lax.dot_general(own.astype(BF16), upto, NN, preferred_element_type=F32)
    sums = jnp.broadcast_to(jnp.sum(own, axis=1, keepdims=True), (frows, LANES))
    before = jnp.where(iota((frows, frows), 1) < iota((frows, frows), 0), 1.0, 0.0).astype(BF16)
    ahead = lax.dot_general(before, sums.astype(BF16), NN, preferred_element_type=F32)
    rk_ref[...] = jnp.where(own > 0.0, inside + ahead - 1.0, -1.0)
    ids = jnp.where(fld2 < 0.0, 0.0, fld2).astype(I32)
    ranks = jnp.where(fld2 < 0.0, -1.0, table_lookup(rk_ref, ids, frows, -1.0))
    sq_ref[...] = jnp.full((LANES, LANES), -1.0, F32)
    sq_ref[0:srows, :] = ranks
    columns = sq_ref[...].T
    hi, mid, lo = split3(z_ref[pl.ds(mine, srows, stride=bands), :])
    places = iota((LANES, owned), 1).astype(F32)
    ones = jnp.ones((1, LANES), F32)
    total = jnp.zeros((SUBS, owned), F32)
    for r in range(srows):
        one_hot = jnp.where(jnp.broadcast_to(columns[:, r : r + 1], (LANES, owned)) == places, 1.0, 0.0)
        lhs = jnp.concatenate([hi[r : r + 1], mid[r : r + 1], lo[r : r + 1], ones, jnp.zeros((4, LANES), F32)], axis=0)
        total = total + lax.dot_general(lhs.astype(BF16), one_hot.astype(BF16), NN, preferred_element_type=F32)
    zp_ref[...] = (total[0:1] + (total[1:2] + total[2:3])) / jnp.maximum(total[3:4], 1.0)


def vmem():
    return pl.BlockSpec(memory_space=pltpu.VMEM)


def smem():
    return pl.BlockSpec(memory_space=pltpu.SMEM)


def move(value, bands, tiles, where):
    pairs = []
    for tile in range(tiles):
        for band in range(bands):
            z, y, x, c = where(tile >> 1, tile & 1, band >> 1, band & 1)
            pairs.append((tile * bands + band, (z * 2 + y) * bands + x * 2 + c))
    return lax.ppermute(value, ("sky", "band"), pairs)


def replicate(payload, bands, tiles):
    layers = tiles // 2
    send = lambda value, where: move(value, bands, tiles, where)
    order = sorted(range(1, layers), key=lambda k: -min(k, layers - k))
    got = {k: send(payload, lambda z, y, x, c, k=k: ((z + k) % layers, y, x, c)) for k in order}
    line = jnp.stack([payload] + [got[k] for k in range(1, layers)])
    beside = send(line, lambda z, y, x, c: (z, y ^ 1, x, c) if c == 0 else (z, y, x ^ 1, c))
    near = jnp.concatenate([line, beside])
    across = send(near, lambda z, y, x, c: (z, y, x ^ 1, c) if c == 0 else (z, y ^ 1, x, c))
    other = lambda z, y, x, c: (z, y, x, c ^ 1)
    return near, across, send(near, other), send(across, other)


def sky_sum(value, bands, tiles):
    value = value + move(value, bands, tiles, lambda z, y, x, c: (z, y ^ 1, x, c))
    step = 1
    while step < tiles // 2:
        value = value + move(value, bands, tiles, lambda z, y, x, c, s=step: (z ^ s, y, x, c))
        step *= 2
    return value


def local_body(magnitudes, weights, slots, block_fields, owner, colors, color_terms):
    bands = color_terms.shape[0]
    tiles = lax.axis_size("sky")
    _, obs, stars = magnitudes.shape
    blocks, entries = block_fields.shape
    fields = owner.shape[0]
    blk_rows = stars // blocks
    owned = fields // tiles
    mags, wts, slt = magnitudes[0], weights[0], slots[0]
    packed = pl.pallas_call(
        pack_kernel,
        name="pack",
        out_shape=jax.ShapeDtypeStruct((2 * obs, stars + LANES), F32),
        in_specs=[vmem()] * 3,
        out_specs=vmem(),
    )(mags, wts, slt)
    raw = lax.all_gather(packed, "band", axis=0)

    rows_dev = (entries + 1) * SUBS
    payload, tab = pl.pallas_call(
        functools.partial(tile_kernel, (bands, obs, stars, blocks, entries, fields, blk_rows)),
        name="tile",
        out_shape=(jax.ShapeDtypeStruct((rows_dev, LANES), F32), jax.ShapeDtypeStruct((SUBS, LANES), I32)),
        in_specs=[smem(), vmem(), vmem(), vmem(), vmem()],
        out_specs=(vmem(), vmem()),
        scratch_shapes=[
            pltpu.VMEM((SUBS, LANES), I32),
            pltpu.VMEM((LANES, LANES), F32),
            pltpu.VMEM((bands * entries, blk_rows), F32),
            pltpu.VMEM((bands * entries, blk_rows), F32),
            pltpu.VMEM((fields // LANES, LANES), F32),
        ],
    )(color_terms, raw, mags, block_fields, colors.reshape(-1, LANES))

    spread = replicate(payload, bands, tiles)

    groups = entries // 4
    pair = 2 * bands
    vrows = groups * pair
    zp, means, partial = pl.pallas_call(
        functools.partial(sweep_kernel, (tiles, bands, obs, stars, blocks, entries, fields, blk_rows, owned)),
        name="sweeps",
        out_shape=(
            jax.ShapeDtypeStruct((1, owned), F32),
            jax.ShapeDtypeStruct((1, stars), F32),
            jax.ShapeDtypeStruct((SUBS, LANES), F32),
        ),
        in_specs=[smem()] + [pl.BlockSpec(memory_space=pl.ANY)] * 4 + [vmem()] * 4,
        out_specs=(vmem(), vmem(), vmem()),
        scratch_shapes=[
            pltpu.VMEM((LANES, LANES), F32),
            pltpu.VMEM((vrows, LANES), F32),
            pltpu.VMEM((vrows, LANES), F32),
            pltpu.VMEM((vrows, LANES), F32),
            pltpu.VMEM((vrows, LANES), F32),
            pltpu.VMEM((bands * entries * vrows, LANES), F32),
            pltpu.VMEM((COLORS * FOLD * FOLD, 2 * LANES, 2 * LANES), BF16),
            pltpu.VMEM((vrows, LANES), F32),
            pltpu.VMEM((bands * entries, LANES), F32),
            pltpu.VMEM((SWEEPS, vrows, LANES), F32),
            pltpu.VMEM((LANES, LANES), F32),
            pltpu.SMEM((2, COLORS), I32),
            pltpu.VMEM((2 * groups, LANES, LANES), F32),
            pltpu.VMEM((2 * groups, SUBS, LANES), F32),
            pltpu.VMEM((vrows, LANES), F32),
            pltpu.VMEM((SWEEPS * bands, SUBS, LANES), F32),
            pltpu.VMEM((fields // LANES, LANES), F32),
            pltpu.VMEM((groups, 4 * bands, 2 * LANES), F32),
            pltpu.VMEM((tiles * bands, rows_dev, LANES), F32),
            pltpu.SemaphoreType.DMA((tiles * bands,)),
        ],
        compiler_params=pltpu.CompilerParams(vmem_limit_bytes=56 * 1024 * 1024),
    )(color_terms, *spread, raw, mags, tab, owner.reshape(-1, LANES))

    misfit = sky_sum(partial[0:1], bands, tiles)[0, :SWEEPS] / (obs * stars * tiles)
    return zp, means, misfit[:, None]


def fits_local(mesh, blocks_all, entries, stars, obs, bands, fields):
    tiles = mesh.shape["sky"]
    blocks = blocks_all // tiles
    return (
        2 * blocks_all == LANES
        and blocks == SUBS
        and bands == 4
        and bands * entries == LANES
        and obs == SUBS
        and 2 * bands == SUBS
        and mesh.shape["band"] == bands
        and stars // tiles == 2 * obs * LANES
        and (stars // blocks_all) % LANES == 0
        and fields % (tiles * LANES) == 0
    )


def from_behind(value, axis, steps):
    count = lax.axis_size(axis)
    pairs = [(source, (source + steps) % count) for source in range(count)]
    return lax.ppermute(value, axis, pairs)


def wide_body(magnitudes, weights, slots, block_fields, owner, colors, color_terms):
    band_count = color_terms.shape[0]
    tiles = lax.axis_size("sky")
    my_tile = lax.axis_index("sky")
    my_band = lax.axis_index("band")
    band_mags, band_wts, band_slots = (magnitudes, weights, slots)
    own_row = 0
    band_rows, obs_count, star_count = band_mags.shape
    block_count, list_len = block_fields.shape
    block_rows = star_count // block_count
    fields = owner.shape[0]
    slot_grid = band_slots.reshape(band_rows, obs_count, block_count, block_rows)
    entries = jnp.arange(list_len, dtype=jnp.int32)
    star_weight = jnp.sum(band_wts, axis=1)
    mixing = (
        jnp.eye(band_count, dtype=jnp.float32)
        + color_terms
        - jnp.diag(jnp.sum(color_terms, axis=1))
    )
    owner_order = jnp.argsort(owner, stable=True)
    owned = fields // tiles

    def slot_sums(values):
        grid = values.reshape(band_rows, obs_count, block_count, block_rows)
        hits = slot_grid[..., None] == entries
        return jnp.sum(jnp.where(hits, grid[..., None], 0.0), axis=(1, 3))

    def spread(list_vals):
        hits = slot_grid[..., None] == entries
        picked = jnp.sum(jnp.where(hits, list_vals[:, None, :, None, :], 0.0), axis=4)
        return picked.reshape(band_rows, obs_count, star_count)

    def predict(zp_obs):
        star_means = jnp.sum(band_wts * (band_mags - zp_obs), axis=1) / star_weight
        all_means = lax.all_gather(star_means, "band", axis=0, tiled=True)
        mix_row = lax.dynamic_index_in_dim(mixing, my_band, 0, keepdims=True)
        predicted = jnp.dot(mix_row, all_means, precision=lax.Precision.HIGHEST)
        return (star_means, predicted)

    positions = jnp.argsort(owner_order, stable=True)
    rank_in = positions - owner * owned
    live = block_fields < fields
    safe_ids = jnp.minimum(block_fields, fields - 1)
    relative = jnp.mod(jnp.take(owner, safe_ids) - my_tile + 1, tiles)
    list_ids = jnp.where(live, relative * owned + jnp.take(rank_in, safe_ids), 3 * owned)
    segments = 3 * owned
    nearby_idx = jnp.mod(my_tile + jnp.arange(3, dtype=jnp.int32) - 1, tiles)
    near_fields = jnp.take(owner_order.reshape(tiles, owned), nearby_idx, axis=0)
    zp_colors = jnp.take(colors, near_fields)[None]
    zero_pts = jnp.zeros((band_rows, 3, owned), jnp.float32)

    def flatten(table):
        return table.reshape(band_rows, 3 * owned)

    def combine(partial_flat):
        partial_sums = partial_flat.reshape(band_rows, 3, owned)
        from_left = from_behind(partial_sums[:, 1:3], "sky", 1)
        from_right = from_behind(partial_sums[:, 0:2], "sky", -1)
        far_left = from_behind(partial_sums[:, 2], "sky", 2)
        far_right = from_behind(partial_sums[:, 0], "sky", -2)
        below = far_left + from_left[:, 0] + partial_sums[:, 0]
        middle = from_left[:, 1] + partial_sums[:, 1] + from_right[:, 0]
        above = partial_sums[:, 2] + from_right[:, 1] + far_right
        return jnp.stack([below, middle, above], axis=1)

    def lookup(table):
        padded = jnp.concatenate([flatten(table), jnp.zeros((band_rows, 1), jnp.float32)], axis=1)
        return spread(jnp.take(padded, list_ids, axis=1))

    def segment_band(per_band):
        return jax.ops.segment_sum(
            per_band.reshape(-1), list_ids.reshape(-1), num_segments=segments + 1
        )[:segments]

    def totals(values):
        per_slot = slot_sums(values)
        return combine(jax.vmap(segment_band)(per_slot))

    denominators = totals(band_wts) + PRIOR_WEIGHT

    def squared_misfit(residual, zp_obs):
        per_band = jnp.sum(band_wts * (residual - zp_obs) ** 2, axis=(1, 2))
        return lax.dynamic_index_in_dim(per_band, own_row, 0, keepdims=False)

    def advance(table, color_no):
        zp_obs = lookup(table)
        star_means, predicted = predict(zp_obs)
        residual = band_mags - predicted[:, None, :]
        updated = totals(band_wts * residual) / denominators
        local_value = squared_misfit(residual, zp_obs)
        return (jnp.where(zp_colors == color_no, updated, table), local_value)

    def later_colors(color_no, table):
        return advance(table, color_no)[0]

    def record(local_value):
        return lax.psum(local_value, "sky")

    recorded = []
    for sweep_no in range(SWEEPS):
        zero_pts, local_value = advance(zero_pts, 0)
        if sweep_no > 0:
            recorded.append(record(local_value))
        zero_pts = lax.fori_loop(1, COLORS, later_colors, zero_pts)
    zp_obs = lookup(zero_pts)
    star_means, predicted = predict(zp_obs)
    residual = band_mags - predicted[:, None, :]
    recorded.append(record(squared_misfit(residual, zp_obs)))
    stacked = jnp.stack(recorded)
    misfit = stacked / (obs_count * star_count * tiles)
    own_zp = lax.dynamic_index_in_dim(zero_pts[:, 1], own_row, 0, keepdims=True)
    own_means = lax.dynamic_index_in_dim(star_means, own_row, 0, keepdims=True)
    return (own_zp, own_means, misfit[:, None])


def solution(mesh):
    in_specs = (
        P("band", None, "sky"),
        P("band", None, "sky"),
        P("band", None, "sky"),
        P("sky", None),
        P(),
        P(),
        P(),
    )
    out_specs = (P("band", "sky"), P("band", "sky"), P(None, "band"))

    def call(magnitudes, weights, slots, block_fields, owner, colors, color_terms):
        bands, obs, stars = magnitudes.shape
        blocks_all, entries = block_fields.shape
        local = fits_local(mesh, blocks_all, entries, stars, obs, bands, owner.shape[0])
        body = local_body if local else wide_body
        run = jax.shard_map(body, mesh=mesh, in_specs=in_specs, out_specs=out_specs, check_vma=False)
        return run(magnitudes, weights, slots, block_fields, owner, colors, color_terms)

    return call
```

```python
import functools

import jax
import jax.numpy as jnp
from jax import lax
from jax.experimental import pallas as pl
from jax.experimental.pallas import tpu as pltpu
from jax.sharding import PartitionSpec as P


COLORS = 8
SWEEPS = 4


PRIOR_WEIGHT = 1.0
LANES = 128
SUBS = 8
HALF = LANES // 2
FOLDS = (2, 3)
MOST = max(FOLDS) ** 2
F32 = jnp.float32
BF16 = jnp.bfloat16
I32 = jnp.int32
NT = (((1,), (1,)), ((), ()))
NN = (((1,), (0,)), ((), ()))


def iota(shape, axis):
    return lax.broadcasted_iota(I32, shape, axis)


def pick(table, idx):
    return jnp.take_along_axis(table, idx, axis=1, mode="promise_in_bounds")


def row_to(value, rows):
    return jnp.broadcast_to(value, (rows, value.shape[1]))


def table_lookup(table_ref, ids, rows, init):
    out = jnp.full(ids.shape, init, F32)
    for r in range(rows):
        hit = pick(row_to(table_ref[r : r + 1, :], ids.shape[0]), ids & (LANES - 1))
        out = jnp.where((ids >> 7) == r, hit, out)
    return out


def mixing_row(terms_ref, mine, bands):
    total = terms_ref[mine, 0]
    for b in range(1, bands):
        total = total + terms_ref[mine, b]
    return [terms_ref[mine, b] + jnp.where(mine == b, 1.0 - total, 0.0) for b in range(bands)]


def pack_kernel(mag_ref, wt_ref, slot_ref, out_ref):
    obs, stars = mag_ref.shape
    w = wt_ref[...]
    out_ref[0:obs, 0:stars] = w
    out_ref[obs : 2 * obs, 0:stars] = slot_ref[...].astype(F32)
    base = jnp.sum(w * mag_ref[...], axis=0, keepdims=True) / jnp.sum(w, axis=0, keepdims=True)
    for i in range(stars // LANES):
        out_ref[i : i + 1, stars : stars + LANES] = base[:, i * LANES : (i + 1) * LANES]


def tile_kernel(
    dims, terms_ref, raw_ref, mag_ref, lists_ref, colors_ref, out0_ref, out1_ref, tab_ref, pad_ref, sq_ref, wf_ref, x_ref, colf_ref
):
    bands, obs, stars, blocks, entries, fields, blk_rows = dims
    lane = iota((SUBS, LANES), 1)
    pad_ref[...] = jnp.full((SUBS, LANES), fields, I32)
    pad_ref[:, :entries] = lists_ref[...]
    ids = pad_ref[...]
    live = ids < fields
    safe = jnp.where(live, ids, 0)
    colf_ref[...] = colors_ref[...].astype(F32)
    color = table_lookup(colf_ref, safe, fields // LANES, 0.0).astype(I32)
    key = jnp.where(live, color * entries + lane, COLORS * entries)
    rank = jnp.zeros((SUBS, LANES), I32)
    for e in range(entries):
        rank = rank + jnp.where(key[:, e : e + 1] < key, 1, 0)
    live_f = jnp.where(live, 1.0, 0.0)
    dead = entries - jnp.sum(live_f, axis=1, keepdims=True).astype(I32)
    pos = jnp.where(live, rank + ((dead * color) >> (COLORS.bit_length() - 1)), 4 * LANES)
    inv = jnp.full((SUBS, LANES), -1, I32)
    for e in range(entries):
        inv = jnp.where(pos[:, e : e + 1] == lane, e, inv)
    used = inv >= 0
    inv_safe = jnp.where(used, inv, 0)
    fpos = jnp.where(used, pick(ids, inv_safe).astype(F32), -1.0)
    cpos = jnp.where(used, pick(color, inv_safe).astype(F32), float(COLORS))
    pos_live = jnp.where(live, pos, 0)
    tab_ref[...] = ((pos_live >> 1) & 1) * HALF + (pos_live >> 2) * (2 * bands) + (pos_live & 1) * bands

    sq_ref[...] = jnp.zeros((LANES, LANES), F32)
    sq_ref[0:SUBS, :] = inv.astype(F32)
    inv_t = sq_ref[...].T
    mine = lax.axis_index("band")
    mix_ref = mixing_row(terms_ref, mine, bands)
    lanes_sq = iota((entries, LANES), 1)
    t0_cols = jnp.zeros((entries, LANES), F32)
    wt_cols = jnp.zeros((entries, LANES), F32)
    for blk in range(blocks):
        lo, hi = blk * blk_rows, (blk + 1) * blk_rows
        inv_col = jnp.broadcast_to(inv_t[0:entries, blk : blk + 1], (entries, blk_rows))
        pred = jnp.zeros((1, blk_rows), F32)
        for b in range(bands):
            w = raw_ref[b, 0:obs, lo:hi]
            slot = raw_ref[b, obs : 2 * obs, lo:hi]
            acc = jnp.zeros((entries, blk_rows), F32)
            for k in range(obs):
                acc = acc + jnp.where(slot[k : k + 1] == inv_col, w[k : k + 1], 0.0)
            scale = mix_ref[b] / jnp.sum(w, axis=0, keepdims=True)
            wf_ref[b * entries : (b + 1) * entries, :] = acc
            x_ref[b * entries : (b + 1) * entries, :] = acc * scale
            pieces = blk_rows // LANES
            means = raw_ref[b, blk * pieces : (blk + 1) * pieces, stars : stars + LANES]
            pred = pred + mix_ref[b] * jnp.concatenate([means[i : i + 1] for i in range(pieces)], axis=1)
        own = wf_ref[pl.ds(mine * entries, entries), :]
        gram = lax.dot_general(own, x_ref[...], NT, precision=lax.Precision.HIGHEST, preferred_element_type=F32)
        cut = entries // 2
        out0_ref[pl.ds(SUBS + blk, cut, stride=SUBS), :] = gram[:cut]
        out1_ref[pl.ds(blk, cut, stride=SUBS), :] = gram[cut:]
        w = raw_ref[mine, 0:obs, lo:hi]
        slot = raw_ref[mine, obs : 2 * obs, lo:hi]
        value = w * (mag_ref[:, lo:hi] - pred)
        acc = jnp.zeros((entries, blk_rows), F32)
        for k in range(obs):
            acc = acc + jnp.where(slot[k : k + 1] == inv_col, value[k : k + 1], 0.0)
        t0_cols = jnp.where(lanes_sq == blk, jnp.sum(acc, axis=1, keepdims=True), t0_cols)
        wt_cols = jnp.where(lanes_sq == blk, jnp.sum(own, axis=1, keepdims=True), wt_cols)
    sq_ref[...] = jnp.zeros((LANES, LANES), F32)
    sq_ref[0:entries, :] = t0_cols
    sq_ref[entries : 2 * entries, :] = wt_cols
    flipped = sq_ref[...].T[0:SUBS]
    extra = jnp.where(lane < 3 * entries, pltpu.roll(fpos, 2 * entries, 1), pltpu.roll(cpos, 3 * entries, 1))
    out0_ref[0:SUBS, :] = jnp.where(lane < 2 * entries, flipped, extra)


def split3(value):
    hi = value.astype(BF16).astype(F32)
    rest = value - hi
    mid = rest.astype(BF16).astype(F32)
    return hi, mid, rest - mid


def sweep_kernel(
    dims, terms_ref, a0_ref, a1_ref, a2_ref, a3_ref, b0_ref, b1_ref, b2_ref, b3_ref, raw_ref, mag_ref, tab_ref, owner_ref,
    zp_ref, means_ref, misfit_ref,
    et_ref, v_ref, den_ref, fld_ref, col_ref, g_ref, s_ref, z_ref, dz_ref, zs_ref,
    sq_ref, lim_ref, fc_ref, fr_ref, tv_ref, ze_ref, rk_ref, big_ref, td_ref,
):
    tiles, bands, obs, stars, _, entries, fields, blk_rows, owned = dims
    groups = entries // 4
    pair = 2 * bands
    vrows = groups * pair
    lane8 = iota((SUBS, LANES), 1)
    low8 = lane8 < HALF
    my_tile, mine = lax.axis_index("sky"), lax.axis_index("band")
    mix_ref = mixing_row(terms_ref, mine, bands)

    layers = tiles // 2
    my_x, my_c = mine >> 1, mine & 1

    def load(swap):
        def block(part, dc, dx, dy, back, rows):
            d1, d2 = (dx, dy) if (dc == 1) != swap else (dy, dx)
            return part[2 * dc + d2][d1 * layers + back, rows, :]

        parts = ((a0_ref, a1_ref, a2_ref, a3_ref), (b0_ref, b1_ref, b2_ref, b3_ref))
        order = [(dy, back) for dy in range(2) for back in range(layers)]
        for dx in range(2):
            for dc in range(2):
                b = (my_x ^ dx) * 2 + (my_c ^ dc)
                sq_ref[...] = jnp.zeros((LANES, LANES), F32)
                for t, (dy, back) in enumerate(order):
                    sq_ref[t * SUBS : (t + 1) * SUBS, :] = block(parts[0], dc, dx, dy, back, slice(0, SUBS))
                et_ref[...] = sq_ref[...].T
                for p in range(2):
                    for q, dest in enumerate((v_ref, den_ref, fld_ref, col_ref)):
                        first = et_ref[pl.ds(q * entries + p, groups, stride=4), :]
                        second = et_ref[pl.ds(q * entries + 2 + p, groups, stride=4), :]
                        dest[pl.ds(p * bands + b, groups, stride=pair), :] = jnp.where(
                            low8, first, pltpu.roll(second, HALF, 1)
                        )

        for h in range(2):

            def turn(i, carry):
                k = i + h * (groups // 2)
                for p in range(2):
                    for dx in range(2):
                        for dc in range(2):
                            b = (my_x ^ dx) * 2 + (my_c ^ dc)
                            rows = []
                            for half in range(2):
                                start = pl.multiple_of((4 * i + 2 * half + p) * SUBS + (SUBS if h == 0 else 0), SUBS)
                                for dy, back in order:
                                    rows.append(block(parts[h], dc, dx, dy, back, pl.ds(start, SUBS)))
                            flipped = jnp.concatenate(rows, axis=0).T
                            for b2 in range(bands):
                                at = pl.ds(b2 * vrows + k * pair + p * bands + b, entries, stride=bands * vrows)
                                g_ref[at, :] = flipped[b2 * entries : (b2 + 1) * entries]
                return carry

            lax.fori_loop(0, groups // 2, turn, 0)

    @pl.when(my_c == 0)
    def load_even():
        load(False)

    @pl.when(my_c != 0)
    def load_odd():
        load(True)

    srows = 2 * groups
    fld2 = fld_ref[pl.ds(0, srows, stride=bands), :]
    col2 = col_ref[pl.ds(0, srows, stride=bands), :]
    row2 = iota((srows, LANES), 0)
    position = 4 * (row2 >> 1) + 2 * jnp.where(iota((srows, LANES), 1) < HALF, 0, 1) + (row2 & 1)
    for c in range(COLORS):
        hit = col2 == float(c)
        lim_ref[0, c] = jnp.min(jnp.where(hit, position, entries))
        lim_ref[1, c] = jnp.max(jnp.where(hit, position + 1, 0))
        count = jnp.sum(jnp.where(hit, 1.0, 0.0), axis=0, keepdims=True)
        lim_ref[2, c] = jnp.max(count + pltpu.roll(count, HALF, 1)).astype(I32)

    def fold_of(c):
        most = lim_ref[2, c]
        bounds = [0] + [4 * fold for fold in FOLDS]
        return [(fold, (most > low) & (most <= high)) for fold, low, high in zip(FOLDS, bounds, bounds[1:])], most > bounds[-1]

    def build_fold(c, fold):
        chosen = jnp.where(col2 == c.astype(F32), fld2, -1.0)
        folded = []
        for m in range(fold):
            for p in range(2):
                best = jnp.full((1, LANES), -1.0, F32)
                for k in range(m, groups, fold):
                    best = jnp.maximum(best, chosen[2 * k + p : 2 * k + p + 1])
                folded.append(best)
        sq_ref[0 : 2 * fold, :] = jnp.concatenate(folded, axis=0)
        columns = sq_ref[...].T
        others = [jnp.where(row < 0.0, -2.0, row) for row in folded]
        for i in range(2 * fold):
            col = jnp.broadcast_to(columns[:, i : i + 1], (LANES, LANES))
            for j in range(2 * fold):
                tile = jnp.where(col == others[j], 1.0, 0.0).astype(BF16)
                m, p, n, r = i // 2, i % 2, j // 2, j % 2
                s_ref[c * MOST + m * fold + n, p * LANES : (p + 1) * LANES, r * LANES : (r + 1) * LANES] = tile

    def build(c, carry):
        for fold, chosen in fold_of(c)[0]:
            pl.when(chosen)(functools.partial(build_fold, c, fold))
        return carry

    lax.fori_loop(0, COLORS, build, 0)

    def spread_rows(value):
        flat = jnp.concatenate([value[0:bands], value[bands:pair]], axis=1)
        hi, mid, lo = split3(flat)
        return jnp.concatenate([hi, mid, lo, jnp.zeros_like(hi)], axis=0).astype(BF16)

    def pack_rows(total):
        flat = total[0:bands] + (total[bands : 2 * bands] + total[2 * bands : 3 * bands])
        return jnp.concatenate([flat[:, :LANES], flat[:, LANES:]], axis=0)

    def same_field(c, work):
        cf = c.astype(F32)
        choices, rest = fold_of(c)

        def fast(fold):
            lhs = []
            for m in range(fold):
                rows_of = []
                for src, _ in work:
                    total = jnp.zeros((pair, LANES), F32)
                    for k in range(m, groups, fold):
                        rows = slice(k * pair, (k + 1) * pair)
                        total = total + jnp.where(col_ref[rows] == cf, src[rows], 0.0)
                    rows_of.append(spread_rows(total))
                lhs.append(jnp.concatenate(rows_of, axis=0))
            for n in range(fold):
                total = jnp.zeros((4 * bands * len(work), 2 * LANES), F32)
                for m in range(fold):
                    total = total + lax.dot_general(
                        lhs[m], s_ref[c * MOST + m * fold + n], NN, preferred_element_type=F32
                    )
                for i, (_, dest) in enumerate(work):
                    packed = pack_rows(total[4 * bands * i : 4 * bands * (i + 1)])
                    for k in range(n, groups, fold):
                        dest[k * pair : (k + 1) * pair, :] = packed

        for fold, chosen in choices:
            pl.when(chosen)(functools.partial(fast, fold))

        @pl.when(rest)
        def general():
            for src, dest in work:
                one_general(cf, src, dest)

    def one_general(cf, src, dest):
        chosen = jnp.where(col2 == cf, fld2, -1.0)
        sq_ref[...] = jnp.full((LANES, LANES), -1.0, F32)
        sq_ref[0:srows, :] = chosen
        columns = sq_ref[...].T
        for i in range(srows):
            fc_ref[i] = jnp.broadcast_to(columns[:, i : i + 1], (LANES, LANES))
            fr_ref[i] = row_to(jnp.where(chosen[i : i + 1] < 0.0, -2.0, chosen[i : i + 1]), SUBS)
        for m in range(groups):
            rows = slice(m * pair, (m + 1) * pair)
            big_ref[m] = spread_rows(jnp.where(col_ref[rows] == cf, src[rows], 0.0)).astype(F32)

        def outer(n, carry):
            def inner(m, total):
                parts = []
                for r in range(2):
                    row = fr_ref[2 * n + r][0:1]
                    upper = jnp.where(fc_ref[2 * m] == row, 1.0, 0.0)
                    lower = jnp.where(fc_ref[2 * m + 1] == row, 1.0, 0.0)
                    lhs = big_ref[m].astype(BF16)
                    parts.append(
                        lax.dot_general(lhs[:, :LANES], upper.astype(BF16), NN, preferred_element_type=F32)
                        + lax.dot_general(lhs[:, LANES:], lower.astype(BF16), NN, preferred_element_type=F32)
                    )
                return total + jnp.concatenate(parts, axis=1)

            total = lax.fori_loop(0, groups, inner, jnp.zeros((4 * bands, 2 * LANES), F32))
            dest[pl.ds(pl.multiple_of(n * pair, pair), pair), :] = pack_rows(total)
            return carry

        lax.fori_loop(0, groups, outer, 0)

    z_ref[...] = jnp.zeros((vrows, LANES), F32)

    def step(opening, n, carry):
        c = n & (COLORS - 1)
        cf = c.astype(F32)
        if opening:
            same_field(c, ((v_ref, tv_ref), (den_ref, td_ref)))
            for k in range(groups):
                rows = slice(k * pair, (k + 1) * pair)
                den_ref[rows] = jnp.where(col_ref[rows] == cf, 1.0 / (td_ref[rows] + PRIOR_WEIGHT), den_ref[rows])
        else:
            same_field(c, ((v_ref, tv_ref),))
        for k in range(groups):
            rows = slice(k * pair, (k + 1) * pair)
            old = z_ref[rows]
            new = jnp.where(col_ref[rows] == cf, tv_ref[rows] * den_ref[rows], old)
            z_ref[rows] = new
            diff = new - old
            turned = pltpu.roll(diff, HALF, 1)
            dz_ref[2 * k * pair : (2 * k + 1) * pair, :] = jnp.where(low8, diff, turned)
            dz_ref[(2 * k + 1) * pair : (2 * k + 2) * pair, :] = jnp.where(low8, turned, diff)

        def apply(q, accs):
            first = q * (2 * bands)
            rows = [row_to(dz_ref[pl.ds(first + i, 1), :], pair) for i in range(2 * bands)]
            out = []
            for k in range(groups):
                terms = []
                for i in range(2 * bands):
                    base = pl.multiple_of((first + i) * vrows + k * pair, pair)
                    terms.append(g_ref[pl.ds(base, pair), :] * rows[i])
                while len(terms) > 1:
                    terms = [terms[i] + terms[i + 1] for i in range(0, len(terms), 2)]
                out.append(accs[k] + terms[0])
            return tuple(out)

        start = tuple(v_ref[k * pair : (k + 1) * pair] for k in range(groups))
        done = lax.fori_loop(lim_ref[0, c] >> 1, (lim_ref[1, c] + 1) >> 1, apply, start)
        for k in range(groups):
            v_ref[k * pair : (k + 1) * pair, :] = done[k]

        @pl.when(c == COLORS - 1)
        def keep():
            zs_ref[n >> (COLORS.bit_length() - 1)] = z_ref[...]

        return carry

    lax.fori_loop(0, COLORS, functools.partial(step, True), 0)
    lax.fori_loop(COLORS, SWEEPS * COLORS, functools.partial(step, False), 0)

    tab = tab_ref[...]
    for sweep in range(SWEEPS):
        sq_ref[...] = jnp.zeros((LANES, LANES), F32)
        sq_ref[0:vrows, :] = zs_ref[sweep]
        et_ref[...] = sq_ref[...].T
        first = et_ref[0:SUBS, :]
        second = et_ref[HALF : HALF + SUBS, :]
        table = jnp.where(low8, first, pltpu.roll(second, HALF, 1))
        for b in range(bands):
            ze_ref[sweep * bands + b] = pick(table, tab + b)

    squares = [jnp.zeros((obs, LANES), F32) for _ in range(SWEEPS)]
    for chunk in range(stars // LANES):
        at = slice(chunk * LANES, (chunk + 1) * LANES)
        blk = chunk * LANES // blk_rows
        pred = [jnp.zeros((1, LANES), F32) for _ in range(SWEEPS)]
        own_mean = jnp.zeros((1, LANES), F32)
        for b in range(bands):
            w = raw_ref[b, 0:obs, at]
            slot = raw_ref[b, obs : 2 * obs, at].astype(I32)
            inverse = 1.0 / jnp.sum(w, axis=0, keepdims=True)
            base = raw_ref[b, chunk : chunk + 1, stars : stars + LANES]
            for sweep in range(SWEEPS):
                seen = pick(row_to(ze_ref[sweep * bands + b, blk : blk + 1, :], obs), slot)
                mean = base - jnp.sum(w * seen, axis=0, keepdims=True) * inverse
                pred[sweep] = pred[sweep] + mix_ref[b] * mean
                if sweep == SWEEPS - 1:
                    own_mean = jnp.where(mine == b, mean, own_mean)
        means_ref[0:1, at] = own_mean
        w = raw_ref[mine, 0:obs, at]
        slot = raw_ref[mine, obs : 2 * obs, at].astype(I32)
        mag = mag_ref[:, at]
        for sweep in range(SWEEPS):
            seen = pick(row_to(ze_ref[sweep * bands + mine, blk : blk + 1, :], obs), slot)
            gap = mag - pred[sweep] - seen
            squares[sweep] = squares[sweep] + w * gap * gap
    result = jnp.zeros((1, LANES), F32)
    for sweep in range(SWEEPS):
        result = jnp.where(lane8[0:1] == sweep, jnp.sum(squares[sweep]), result)
    misfit_ref[...] = result

    frows = fields // LANES
    own = jnp.where(owner_ref[...] == my_tile, 1.0, 0.0)
    upto = jnp.where(iota((LANES, LANES), 0) <= iota((LANES, LANES), 1), 1.0, 0.0).astype(BF16)
    inside = lax.dot_general(own.astype(BF16), upto, NN, preferred_element_type=F32)
    sums = jnp.broadcast_to(jnp.sum(own, axis=1, keepdims=True), (frows, LANES))
    before = jnp.where(iota((frows, frows), 1) < iota((frows, frows), 0), 1.0, 0.0).astype(BF16)
    ahead = lax.dot_general(before, sums.astype(BF16), NN, preferred_element_type=F32)
    rk_ref[...] = jnp.where(own > 0.0, inside + ahead - 1.0, -1.0)
    ids = jnp.where(fld2 < 0.0, 0.0, fld2).astype(I32)
    ranks = jnp.where(fld2 < 0.0, -1.0, table_lookup(rk_ref, ids, frows, -1.0))
    sq_ref[...] = jnp.full((LANES, LANES), -1.0, F32)
    sq_ref[0:srows, :] = ranks
    columns = sq_ref[...].T
    hi, mid, lo = split3(z_ref[pl.ds(mine, srows, stride=bands), :])
    places = iota((LANES, owned), 1).astype(F32)
    ones = jnp.ones((1, LANES), F32)
    total = jnp.zeros((SUBS, owned), F32)
    for r in range(srows):
        one_hot = jnp.where(jnp.broadcast_to(columns[:, r : r + 1], (LANES, owned)) == places, 1.0, 0.0)
        lhs = jnp.concatenate([hi[r : r + 1], mid[r : r + 1], lo[r : r + 1], ones, jnp.zeros((4, LANES), F32)], axis=0)
        total = total + lax.dot_general(lhs.astype(BF16), one_hot.astype(BF16), NN, preferred_element_type=F32)
    zp_ref[...] = (total[0:1] + (total[1:2] + total[2:3])) / jnp.maximum(total[3:4], 1.0)


def vmem():
    return pl.BlockSpec(memory_space=pltpu.VMEM)


def smem():
    return pl.BlockSpec(memory_space=pltpu.SMEM)


def move(value, bands, tiles, where):
    pairs = []
    for tile in range(tiles):
        for band in range(bands):
            z, y, x, c = where(tile >> 1, tile & 1, band >> 1, band & 1)
            pairs.append((tile * bands + band, (z * 2 + y) * bands + x * 2 + c))
    return lax.ppermute(value, ("sky", "band"), pairs)


def replicate(halves, bands, tiles):
    layers = tiles // 2
    send = lambda value, where: move(value, bands, tiles, where)
    order = sorted(range(1, layers), key=lambda k: -min(k, layers - k))
    other = lambda z, y, x, c: (z, y, x, c ^ 1)
    spread = []
    for half in halves:
        got = {k: send(half, lambda z, y, x, c, k=k: ((z + k) % layers, y, x, c)) for k in order}
        line = jnp.stack([half] + [got[k] for k in range(1, layers)])
        beside = send(line, lambda z, y, x, c: (z, y ^ 1, x, c) if c == 0 else (z, y, x ^ 1, c))
        near = jnp.concatenate([line, beside])
        across = send(near, lambda z, y, x, c: (z, y, x ^ 1, c) if c == 0 else (z, y ^ 1, x, c))
        spread += [near, across, send(near, other), send(across, other)]
    return spread


def sky_sum(value, bands, tiles):
    value = value + move(value, bands, tiles, lambda z, y, x, c: (z, y ^ 1, x, c))
    step = 1
    while step < tiles // 2:
        value = value + move(value, bands, tiles, lambda z, y, x, c, s=step: (z ^ s, y, x, c))
        step *= 2
    return value


def local_body(magnitudes, weights, slots, block_fields, owner, colors, color_terms):
    bands = color_terms.shape[0]
    tiles = lax.axis_size("sky")
    _, obs, stars = magnitudes.shape
    blocks, entries = block_fields.shape
    fields = owner.shape[0]
    blk_rows = stars // blocks
    owned = fields // tiles
    mags, wts, slt = magnitudes[0], weights[0], slots[0]
    packed = pl.pallas_call(
        pack_kernel,
        name="pack",
        out_shape=jax.ShapeDtypeStruct((2 * obs, stars + LANES), F32),
        in_specs=[vmem()] * 3,
        out_specs=vmem(),
    )(mags, wts, slt)
    raw = lax.all_gather(packed, "band", axis=0)

    rows_half = entries * SUBS // 2
    first, second, tab = pl.pallas_call(
        functools.partial(tile_kernel, (bands, obs, stars, blocks, entries, fields, blk_rows)),
        name="tile",
        out_shape=(
            jax.ShapeDtypeStruct((rows_half + SUBS, LANES), F32),
            jax.ShapeDtypeStruct((rows_half, LANES), F32),
            jax.ShapeDtypeStruct((SUBS, LANES), I32),
        ),
        in_specs=[smem(), vmem(), vmem(), vmem(), vmem()],
        out_specs=(vmem(), vmem(), vmem()),
        scratch_shapes=[
            pltpu.VMEM((SUBS, LANES), I32),
            pltpu.VMEM((LANES, LANES), F32),
            pltpu.VMEM((bands * entries, blk_rows), F32),
            pltpu.VMEM((bands * entries, blk_rows), F32),
            pltpu.VMEM((fields // LANES, LANES), F32),
        ],
    )(color_terms, raw, mags, block_fields, colors.reshape(-1, LANES))

    spread = replicate((first, second), bands, tiles)

    groups = entries // 4
    pair = 2 * bands
    vrows = groups * pair
    zp, means, partial = pl.pallas_call(
        functools.partial(sweep_kernel, (tiles, bands, obs, stars, blocks, entries, fields, blk_rows, owned)),
        name="sweeps",
        out_shape=(
            jax.ShapeDtypeStruct((1, owned), F32),
            jax.ShapeDtypeStruct((1, stars), F32),
            jax.ShapeDtypeStruct((1, LANES), F32),
        ),
        in_specs=[smem()] + [vmem()] * 12,
        out_specs=(vmem(), vmem(), vmem()),
        scratch_shapes=[
            pltpu.VMEM((LANES, LANES), F32),
            pltpu.VMEM((vrows, LANES), F32),
            pltpu.VMEM((vrows, LANES), F32),
            pltpu.VMEM((vrows, LANES), F32),
            pltpu.VMEM((vrows, LANES), F32),
            pltpu.VMEM((bands * entries * vrows, LANES), F32),
            pltpu.VMEM((COLORS * MOST, 2 * LANES, 2 * LANES), BF16),
            pltpu.VMEM((vrows, LANES), F32),
            pltpu.VMEM((bands * entries, LANES), F32),
            pltpu.VMEM((SWEEPS, vrows, LANES), F32),
            pltpu.VMEM((LANES, LANES), F32),
            pltpu.SMEM((3, COLORS), I32),
            pltpu.VMEM((2 * groups, LANES, LANES), F32),
            pltpu.VMEM((2 * groups, SUBS, LANES), F32),
            pltpu.VMEM((vrows, LANES), F32),
            pltpu.VMEM((SWEEPS * bands, SUBS, LANES), F32),
            pltpu.VMEM((fields // LANES, LANES), F32),
            pltpu.VMEM((groups, 4 * bands, 2 * LANES), F32),
            pltpu.VMEM((vrows, LANES), F32),
        ],
        compiler_params=pltpu.CompilerParams(vmem_limit_bytes=32 * 1024 * 1024),
    )(color_terms, *spread, raw, mags, tab, owner.reshape(-1, LANES))

    misfit = sky_sum(partial, bands, tiles)[0, :SWEEPS] / (obs * stars * tiles)
    return zp, means, misfit[:, None]


def fits_local(mesh, blocks_all, entries, stars, obs, bands, fields):
    tiles = mesh.shape["sky"]
    blocks = blocks_all // tiles
    return (
        2 * blocks_all == LANES
        and blocks == SUBS
        and bands == 4
        and bands * entries == LANES
        and obs == SUBS
        and 2 * bands == SUBS
        and mesh.shape["band"] == bands
        and stars // tiles == 2 * obs * LANES
        and (stars // blocks_all) % LANES == 0
        and fields % (tiles * LANES) == 0
    )


def from_behind(value, axis, steps):
    count = lax.axis_size(axis)
    pairs = [(source, (source + steps) % count) for source in range(count)]
    return lax.ppermute(value, axis, pairs)


def wide_body(magnitudes, weights, slots, block_fields, owner, colors, color_terms):
    band_count = color_terms.shape[0]
    tiles = lax.axis_size("sky")
    my_tile = lax.axis_index("sky")
    my_band = lax.axis_index("band")
    band_mags, band_wts, band_slots = (magnitudes, weights, slots)
    own_row = 0
    band_rows, obs_count, star_count = band_mags.shape
    block_count, list_len = block_fields.shape
    block_rows = star_count // block_count
    fields = owner.shape[0]
    slot_grid = band_slots.reshape(band_rows, obs_count, block_count, block_rows)
    entries = jnp.arange(list_len, dtype=jnp.int32)
    star_weight = jnp.sum(band_wts, axis=1)
    mixing = (
        jnp.eye(band_count, dtype=jnp.float32)
        + color_terms
        - jnp.diag(jnp.sum(color_terms, axis=1))
    )
    owner_order = jnp.argsort(owner, stable=True)
    owned = fields // tiles

    def slot_sums(values):
        grid = values.reshape(band_rows, obs_count, block_count, block_rows)
        hits = slot_grid[..., None] == entries
        return jnp.sum(jnp.where(hits, grid[..., None], 0.0), axis=(1, 3))

    def spread(list_vals):
        hits = slot_grid[..., None] == entries
        picked = jnp.sum(jnp.where(hits, list_vals[:, None, :, None, :], 0.0), axis=4)
        return picked.reshape(band_rows, obs_count, star_count)

    def predict(zp_obs):
        star_means = jnp.sum(band_wts * (band_mags - zp_obs), axis=1) / star_weight
        all_means = lax.all_gather(star_means, "band", axis=0, tiled=True)
        mix_row = lax.dynamic_index_in_dim(mixing, my_band, 0, keepdims=True)
        predicted = jnp.dot(mix_row, all_means, precision=lax.Precision.HIGHEST)
        return (star_means, predicted)

    positions = jnp.argsort(owner_order, stable=True)
    rank_in = positions - owner * owned
    live = block_fields < fields
    safe_ids = jnp.minimum(block_fields, fields - 1)
    relative = jnp.mod(jnp.take(owner, safe_ids) - my_tile + 1, tiles)
    list_ids = jnp.where(live, relative * owned + jnp.take(rank_in, safe_ids), 3 * owned)
    segments = 3 * owned
    nearby_idx = jnp.mod(my_tile + jnp.arange(3, dtype=jnp.int32) - 1, tiles)
    near_fields = jnp.take(owner_order.reshape(tiles, owned), nearby_idx, axis=0)
    zp_colors = jnp.take(colors, near_fields)[None]
    zero_pts = jnp.zeros((band_rows, 3, owned), jnp.float32)

    def flatten(table):
        return table.reshape(band_rows, 3 * owned)

    def combine(partial_flat):
        partial_sums = partial_flat.reshape(band_rows, 3, owned)
        from_left = from_behind(partial_sums[:, 1:3], "sky", 1)
        from_right = from_behind(partial_sums[:, 0:2], "sky", -1)
        far_left = from_behind(partial_sums[:, 2], "sky", 2)
        far_right = from_behind(partial_sums[:, 0], "sky", -2)
        below = far_left + from_left[:, 0] + partial_sums[:, 0]
        middle = from_left[:, 1] + partial_sums[:, 1] + from_right[:, 0]
        above = partial_sums[:, 2] + from_right[:, 1] + far_right
        return jnp.stack([below, middle, above], axis=1)

    def lookup(table):
        padded = jnp.concatenate([flatten(table), jnp.zeros((band_rows, 1), jnp.float32)], axis=1)
        return spread(jnp.take(padded, list_ids, axis=1))

    def segment_band(per_band):
        return jax.ops.segment_sum(
            per_band.reshape(-1), list_ids.reshape(-1), num_segments=segments + 1
        )[:segments]

    def totals(values):
        per_slot = slot_sums(values)
        return combine(jax.vmap(segment_band)(per_slot))

    denominators = totals(band_wts) + PRIOR_WEIGHT

    def squared_misfit(residual, zp_obs):
        per_band = jnp.sum(band_wts * (residual - zp_obs) ** 2, axis=(1, 2))
        return lax.dynamic_index_in_dim(per_band, own_row, 0, keepdims=False)

    def advance(table, color_no):
        zp_obs = lookup(table)
        _, predicted = predict(zp_obs)
        residual = band_mags - predicted[:, None, :]
        updated = totals(band_wts * residual) / denominators
        local_value = squared_misfit(residual, zp_obs)
        return (jnp.where(zp_colors == color_no, updated, table), local_value)

    def later_colors(color_no, table):
        return advance(table, color_no)[0]

    def record(local_value):
        return lax.psum(local_value, "sky")

    recorded = []
    for sweep_no in range(SWEEPS):
        zero_pts, local_value = advance(zero_pts, 0)
        if sweep_no > 0:
            recorded.append(record(local_value))
        zero_pts = lax.fori_loop(1, COLORS, later_colors, zero_pts)
    zp_obs = lookup(zero_pts)
    star_means, predicted = predict(zp_obs)
    residual = band_mags - predicted[:, None, :]
    recorded.append(record(squared_misfit(residual, zp_obs)))
    stacked = jnp.stack(recorded)
    misfit = stacked / (obs_count * star_count * tiles)
    own_zp = lax.dynamic_index_in_dim(zero_pts[:, 1], own_row, 0, keepdims=True)
    own_means = lax.dynamic_index_in_dim(star_means, own_row, 0, keepdims=True)
    return (own_zp, own_means, misfit[:, None])


def solution(mesh):
    in_specs = (
        P("band", None, "sky"),
        P("band", None, "sky"),
        P("band", None, "sky"),
        P("sky", None),
        P(),
        P(),
        P(),
    )
    out_specs = (P("band", "sky"), P("band", "sky"), P(None, "band"))

    def call(magnitudes, weights, slots, block_fields, owner, colors, color_terms):
        bands, obs, stars = magnitudes.shape
        blocks_all, entries = block_fields.shape
        local = fits_local(mesh, blocks_all, entries, stars, obs, bands, owner.shape[0])
        body = local_body if local else wide_body
        run = jax.shard_map(body, mesh=mesh, in_specs=in_specs, out_specs=out_specs, check_vma=False)
        return run(magnitudes, weights, slots, block_fields, owner, colors, color_terms)

    return call
```

```python
import functools

import jax
import jax.numpy as jnp
from jax import lax
from jax.experimental import pallas as pl
from jax.experimental.pallas import tpu as pltpu
from jax.sharding import PartitionSpec as P


COLORS = 8
SWEEPS = 4


PRIOR_WEIGHT = 1.0
LANES = 128
SUBS = 8
HALF = LANES // 2
FOLDS = (2, 3)
MOST = max(FOLDS) ** 2
F32 = jnp.float32
BF16 = jnp.bfloat16
I32 = jnp.int32
NT = (((1,), (1,)), ((), ()))
NN = (((1,), (0,)), ((), ()))


def iota(shape, axis):
    return lax.broadcasted_iota(I32, shape, axis)


def pick(table, idx):
    return jnp.take_along_axis(table, idx, axis=1, mode="promise_in_bounds")


def row_to(value, rows):
    return jnp.broadcast_to(value, (rows, value.shape[1]))


def table_lookup(table_ref, ids, rows, init):
    out = jnp.full(ids.shape, init, F32)
    for r in range(rows):
        hit = pick(row_to(table_ref[r : r + 1, :], ids.shape[0]), ids & (LANES - 1))
        out = jnp.where((ids >> 7) == r, hit, out)
    return out


def mixing_row(terms_ref, mine, bands):
    total = terms_ref[mine, 0]
    for b in range(1, bands):
        total = total + terms_ref[mine, b]
    return [terms_ref[mine, b] + jnp.where(mine == b, 1.0 - total, 0.0) for b in range(bands)]


def pack_kernel(mag_ref, wt_ref, slot_ref, out_ref):
    obs, stars = mag_ref.shape
    w = wt_ref[...]
    out_ref[0:obs, 0:stars] = w
    out_ref[obs : 2 * obs, 0:stars] = slot_ref[...].astype(F32)
    base = jnp.sum(w * mag_ref[...], axis=0, keepdims=True) / jnp.sum(w, axis=0, keepdims=True)
    for i in range(stars // LANES):
        out_ref[i : i + 1, stars : stars + LANES] = base[:, i * LANES : (i + 1) * LANES]


def tile_kernel(
    dims, terms_ref, raw_ref, mag_ref, lists_ref, colors_ref, out0_ref, out1_ref, tab_ref, pad_ref, sq_ref, wf_ref, x_ref, colf_ref
):
    bands, obs, stars, blocks, entries, fields, blk_rows = dims
    lane = iota((SUBS, LANES), 1)
    pad_ref[...] = jnp.full((SUBS, LANES), fields, I32)
    pad_ref[:, :entries] = lists_ref[...]
    ids = pad_ref[...]
    live = ids < fields
    safe = jnp.where(live, ids, 0)
    colf_ref[...] = colors_ref[...].astype(F32)
    color = table_lookup(colf_ref, safe, fields // LANES, 0.0).astype(I32)
    key = jnp.where(live, color * entries + lane, COLORS * entries)
    rank = jnp.zeros((SUBS, LANES), I32)
    for e in range(entries):
        rank = rank + jnp.where(key[:, e : e + 1] < key, 1, 0)
    live_f = jnp.where(live, 1.0, 0.0)
    dead = entries - jnp.sum(live_f, axis=1, keepdims=True).astype(I32)
    pos = jnp.where(live, rank + ((dead * color) >> (COLORS.bit_length() - 1)), 4 * LANES)
    inv = jnp.full((SUBS, LANES), -1, I32)
    for e in range(entries):
        inv = jnp.where(pos[:, e : e + 1] == lane, e, inv)
    used = inv >= 0
    inv_safe = jnp.where(used, inv, 0)
    fpos = jnp.where(used, pick(ids, inv_safe).astype(F32), -1.0)
    cpos = jnp.where(used, pick(color, inv_safe).astype(F32), float(COLORS))
    pos_live = jnp.where(live, pos, 0)
    tab_ref[...] = ((pos_live >> 1) & 1) * HALF + (pos_live >> 2) * (2 * bands) + (pos_live & 1) * bands

    sq_ref[...] = jnp.zeros((LANES, LANES), F32)
    sq_ref[0:SUBS, :] = inv.astype(F32)
    inv_t = sq_ref[...].T
    mine = lax.axis_index("band")
    mix_ref = mixing_row(terms_ref, mine, bands)
    lanes_sq = iota((entries, LANES), 1)
    t0_cols = jnp.zeros((entries, LANES), F32)
    wt_cols = jnp.zeros((entries, LANES), F32)
    for blk in range(blocks):
        lo, hi = blk * blk_rows, (blk + 1) * blk_rows
        inv_col = jnp.broadcast_to(inv_t[0:entries, blk : blk + 1], (entries, blk_rows))
        pred = jnp.zeros((1, blk_rows), F32)
        for b in range(bands):
            w = raw_ref[b, 0:obs, lo:hi]
            slot = raw_ref[b, obs : 2 * obs, lo:hi]
            acc = jnp.zeros((entries, blk_rows), F32)
            for k in range(obs):
                acc = acc + jnp.where(slot[k : k + 1] == inv_col, w[k : k + 1], 0.0)
            scale = mix_ref[b] / jnp.sum(w, axis=0, keepdims=True)
            wf_ref[b * entries : (b + 1) * entries, :] = acc
            x_ref[b * entries : (b + 1) * entries, :] = acc * scale
            pieces = blk_rows // LANES
            means = raw_ref[b, blk * pieces : (blk + 1) * pieces, stars : stars + LANES]
            pred = pred + mix_ref[b] * jnp.concatenate([means[i : i + 1] for i in range(pieces)], axis=1)
        own = wf_ref[pl.ds(mine * entries, entries), :]
        gram = lax.dot_general(own, x_ref[...], NT, precision=lax.Precision.HIGHEST, preferred_element_type=F32)
        cut = entries // 2
        out0_ref[pl.ds(SUBS + blk, cut, stride=SUBS), :] = gram[:cut]
        out1_ref[pl.ds(blk, cut, stride=SUBS), :] = gram[cut:]
        w = raw_ref[mine, 0:obs, lo:hi]
        slot = raw_ref[mine, obs : 2 * obs, lo:hi]
        value = w * (mag_ref[:, lo:hi] - pred)
        acc = jnp.zeros((entries, blk_rows), F32)
        for k in range(obs):
            acc = acc + jnp.where(slot[k : k + 1] == inv_col, value[k : k + 1], 0.0)
        t0_cols = jnp.where(lanes_sq == blk, jnp.sum(acc, axis=1, keepdims=True), t0_cols)
        wt_cols = jnp.where(lanes_sq == blk, jnp.sum(own, axis=1, keepdims=True), wt_cols)
    sq_ref[...] = jnp.zeros((LANES, LANES), F32)
    sq_ref[0:entries, :] = t0_cols
    sq_ref[entries : 2 * entries, :] = wt_cols
    flipped = sq_ref[...].T[0:SUBS]
    extra = jnp.where(lane < 3 * entries, pltpu.roll(fpos, 2 * entries, 1), pltpu.roll(cpos, 3 * entries, 1))
    out1_ref[entries * SUBS // 2 :, :] = jnp.zeros((2 * SUBS, LANES), F32)
    out0_ref[0:SUBS, :] = jnp.where(lane < 2 * entries, flipped, extra)


def split3(value):
    hi = value.astype(BF16).astype(F32)
    rest = value - hi
    mid = rest.astype(BF16).astype(F32)
    return hi, mid, rest - mid


def tile_order(tiles):
    return [(dy, back) for dy in range(2) for back in range(tiles // 2)]


def gathered(part, swap, layers, dc, dx, dy, back, rows):
    d1, d2 = (dx, dy) if (dc == 1) != swap else (dy, dx)
    return part[2 * dc + d2][d1 * layers + back, rows, :]


def by_core(mine, run):
    pl.when((mine & 1) == 0)(functools.partial(run, False))
    pl.when((mine & 1) != 0)(functools.partial(run, True))


def turn_half(part, swap, mine, tiles, bands, entries, skip, dest_ref):
    groups = entries // 8
    pair = 2 * bands
    vrows = groups * pair

    def turn(k, carry):
        for p in range(2):
            for dx in range(2):
                for dc in range(2):
                    b = ((mine >> 1) ^ dx) * 2 + ((mine & 1) ^ dc)
                    rows = []
                    for half in range(2):
                        start = pl.multiple_of((4 * k + 2 * half + p) * SUBS + skip, SUBS)
                        for dy, back in tile_order(tiles):
                            rows.append(gathered(part, swap, tiles // 2, dc, dx, dy, back, pl.ds(start, SUBS)))
                    flipped = jnp.concatenate(rows, axis=0).T
                    for b2 in range(bands):
                        at = pl.ds(b2 * vrows + k * pair + p * bands + b, entries, stride=bands * vrows)
                        dest_ref[at, :] = flipped[b2 * entries : (b2 + 1) * entries]
        return carry

    lax.fori_loop(0, groups, turn, 0)


def fold_of(lim_ref, c):
    most = lim_ref[2, c]
    bounds = [0] + [4 * fold for fold in FOLDS]
    return [(fold, (most > low) & (most <= high)) for fold, low, high in zip(FOLDS, bounds, bounds[1:])], most > bounds[-1]


def side_kernel(dims, terms_ref, owner_ref, raw_in, mag_in, tab_in, keep_ref):
    bands, fields, stars = dims
    raw_rows = raw_in.shape[1]
    base = bands * raw_rows
    for b in range(bands):
        keep_ref[b * raw_rows : (b + 1) * raw_rows, :] = raw_in[b]
    keep_ref[base : base + SUBS, 0:stars] = mag_in[...]
    keep_ref[base : base + SUBS, stars : stars + LANES] = tab_in[...].astype(F32)
    low = base + SUBS
    span = fields // LANES // SUBS
    for b, value in enumerate(mixing_row(terms_ref, lax.axis_index("band"), bands)):
        keep_ref[low : low + SUBS, (span + b) * LANES : (span + b + 1) * LANES] = jnp.full((SUBS, LANES), value, F32)
    my_tile = lax.axis_index("sky")
    frows = fields // LANES
    own = jnp.where(owner_ref[...] == my_tile, 1.0, 0.0)
    upto = jnp.where(iota((LANES, LANES), 0) <= iota((LANES, LANES), 1), 1.0, 0.0).astype(BF16)
    inside = lax.dot_general(own.astype(BF16), upto, NN, preferred_element_type=F32)
    sums = jnp.broadcast_to(jnp.sum(own, axis=1, keepdims=True), (frows, LANES))
    before = jnp.where(iota((frows, frows), 1) < iota((frows, frows), 0), 1.0, 0.0).astype(BF16)
    ahead = lax.dot_general(before, sums.astype(BF16), NN, preferred_element_type=F32)
    ranks = jnp.where(own > 0.0, inside + ahead - 1.0, -1.0)
    for i in range(span):
        keep_ref[low : low + SUBS, i * LANES : (i + 1) * LANES] = ranks[i * SUBS : (i + 1) * SUBS]


def ready_kernel(
    dims, near_ref, across_ref, far_near_ref, far_across_ref,
    v_ref, den_ref, fld_ref, col_ref, g_ref, s_ref, lim_ref, sq_ref, et_ref,
):
    tiles, bands, entries = dims
    groups = entries // 4
    pair = 2 * bands
    low8 = iota((SUBS, LANES), 1) < HALF
    mine = lax.axis_index("band")
    part = (near_ref, across_ref, far_near_ref, far_across_ref)

    def load(swap):
        for dx in range(2):
            for dc in range(2):
                b = ((mine >> 1) ^ dx) * 2 + ((mine & 1) ^ dc)
                sq_ref[...] = jnp.zeros((LANES, LANES), F32)
                for t, (dy, back) in enumerate(tile_order(tiles)):
                    sq_ref[t * SUBS : (t + 1) * SUBS, :] = gathered(
                        part, swap, tiles // 2, dc, dx, dy, back, slice(0, SUBS)
                    )
                et_ref[...] = sq_ref[...].T
                for p in range(2):
                    for q, dest in enumerate((v_ref, den_ref, fld_ref, col_ref)):
                        first = et_ref[pl.ds(q * entries + p, groups, stride=4), :]
                        second = et_ref[pl.ds(q * entries + 2 + p, groups, stride=4), :]
                        dest[pl.ds(p * bands + b, groups, stride=pair), :] = jnp.where(
                            low8, first, pltpu.roll(second, HALF, 1)
                        )
        turn_half(part, swap, mine, tiles, bands, entries, SUBS, g_ref)

    by_core(mine, load)
    srows = 2 * groups
    fld2 = fld_ref[pl.ds(0, srows, stride=bands), :]
    col2 = col_ref[pl.ds(0, srows, stride=bands), :]
    row2 = iota((srows, LANES), 0)
    position = 4 * (row2 >> 1) + 2 * jnp.where(iota((srows, LANES), 1) < HALF, 0, 1) + (row2 & 1)
    for c in range(COLORS):
        hit = col2 == float(c)
        lim_ref[0, c] = jnp.min(jnp.where(hit, position, entries))
        lim_ref[1, c] = jnp.max(jnp.where(hit, position + 1, 0))
        count = jnp.sum(jnp.where(hit, 1.0, 0.0), axis=0, keepdims=True)
        lim_ref[2, c] = jnp.max(count + pltpu.roll(count, HALF, 1)).astype(I32)

    def build_fold(c, fold):
        chosen = jnp.where(col2 == c.astype(F32), fld2, -1.0)
        folded = []
        for m in range(fold):
            for p in range(2):
                best = jnp.full((1, LANES), -1.0, F32)
                for k in range(m, groups, fold):
                    best = jnp.maximum(best, chosen[2 * k + p : 2 * k + p + 1])
                folded.append(best)
        sq_ref[0 : 2 * fold, :] = jnp.concatenate(folded, axis=0)
        columns = sq_ref[...].T
        others = [jnp.where(row < 0.0, -2.0, row) for row in folded]
        for i in range(2 * fold):
            col = jnp.broadcast_to(columns[:, i : i + 1], (LANES, LANES))
            for j in range(2 * fold):
                tile = jnp.where(col == others[j], 1.0, 0.0).astype(BF16)
                m, p, n, r = i // 2, i % 2, j // 2, j % 2
                s_ref[c * MOST + m * fold + n, p * LANES : (p + 1) * LANES, r * LANES : (r + 1) * LANES] = tile

    def build(c, carry):
        for fold, chosen in fold_of(lim_ref, c)[0]:
            pl.when(chosen)(functools.partial(build_fold, c, fold))
        return carry

    lax.fori_loop(0, COLORS, build, 0)


def sweep_kernel(
    dims, lim_ref, near_ref, across_ref, far_near_ref, far_across_ref,
    v0_ref, wsum_ref, fld_ref, col_ref, ga_ref, s_ref, keep_ref,
    zp_ref, means_ref, misfit_ref,
    et_ref, v_ref, den_ref, gb_ref, z_ref, dz_ref, zs_ref,
    sq_ref, fc_ref, fr_ref, tv_ref, ze_ref, big_ref, td_ref, rk_ref,
):
    tiles, bands, obs, stars, _, entries, fields, blk_rows, owned = dims
    groups = entries // 4
    pair = 2 * bands
    vrows = groups * pair
    lane8 = iota((SUBS, LANES), 1)
    low8 = lane8 < HALF
    mine = lax.axis_index("band")
    base_row = 2 * obs * bands
    span = fields // LANES // SUBS
    part = (near_ref, across_ref, far_near_ref, far_across_ref)
    by_core(mine, lambda swap: turn_half(part, swap, mine, tiles, bands, entries, 0, gb_ref))
    v_ref[...] = v0_ref[...]
    den_ref[...] = wsum_ref[...]
    srows = 2 * groups
    fld2 = fld_ref[pl.ds(0, srows, stride=bands), :]
    col2 = col_ref[pl.ds(0, srows, stride=bands), :]

    def spread_rows(value):
        flat = jnp.concatenate([value[0:bands], value[bands:pair]], axis=1)
        hi, mid, lo = split3(flat)
        return jnp.concatenate([hi, mid, lo, jnp.zeros_like(hi)], axis=0).astype(BF16)

    def pack_rows(total):
        flat = total[0:bands] + (total[bands : 2 * bands] + total[2 * bands : 3 * bands])
        return jnp.concatenate([flat[:, :LANES], flat[:, LANES:]], axis=0)

    def same_field(c, work):
        cf = c.astype(F32)
        choices, rest = fold_of(lim_ref, c)

        def fast(fold):
            lhs = []
            for m in range(fold):
                rows_of = []
                for src, _ in work:
                    total = jnp.zeros((pair, LANES), F32)
                    for k in range(m, groups, fold):
                        rows = slice(k * pair, (k + 1) * pair)
                        total = total + jnp.where(col_ref[rows] == cf, src[rows], 0.0)
                    rows_of.append(spread_rows(total))
                lhs.append(jnp.concatenate(rows_of, axis=0))
            for n in range(fold):
                total = jnp.zeros((4 * bands * len(work), 2 * LANES), F32)
                for m in range(fold):
                    total = total + lax.dot_general(
                        lhs[m], s_ref[c * MOST + m * fold + n], NN, preferred_element_type=F32
                    )
                for i, (_, dest) in enumerate(work):
                    packed = pack_rows(total[4 * bands * i : 4 * bands * (i + 1)])
                    for k in range(n, groups, fold):
                        dest[k * pair : (k + 1) * pair, :] = packed

        for fold, chosen in choices:
            pl.when(chosen)(functools.partial(fast, fold))

        @pl.when(rest)
        def general():
            for src, dest in work:
                one_general(cf, src, dest)

    def one_general(cf, src, dest):
        chosen = jnp.where(col2 == cf, fld2, -1.0)
        sq_ref[...] = jnp.full((LANES, LANES), -1.0, F32)
        sq_ref[0:srows, :] = chosen
        columns = sq_ref[...].T
        for i in range(srows):
            fc_ref[i] = jnp.broadcast_to(columns[:, i : i + 1], (LANES, LANES))
            fr_ref[i] = row_to(jnp.where(chosen[i : i + 1] < 0.0, -2.0, chosen[i : i + 1]), SUBS)
        for m in range(groups):
            rows = slice(m * pair, (m + 1) * pair)
            big_ref[m] = spread_rows(jnp.where(col_ref[rows] == cf, src[rows], 0.0)).astype(F32)

        def outer(n, carry):
            def inner(m, total):
                parts = []
                for r in range(2):
                    row = fr_ref[2 * n + r][0:1]
                    upper = jnp.where(fc_ref[2 * m] == row, 1.0, 0.0)
                    lower = jnp.where(fc_ref[2 * m + 1] == row, 1.0, 0.0)
                    lhs = big_ref[m].astype(BF16)
                    parts.append(
                        lax.dot_general(lhs[:, :LANES], upper.astype(BF16), NN, preferred_element_type=F32)
                        + lax.dot_general(lhs[:, LANES:], lower.astype(BF16), NN, preferred_element_type=F32)
                    )
                return total + jnp.concatenate(parts, axis=1)

            total = lax.fori_loop(0, groups, inner, jnp.zeros((4 * bands, 2 * LANES), F32))
            dest[pl.ds(pl.multiple_of(n * pair, pair), pair), :] = pack_rows(total)
            return carry

        lax.fori_loop(0, groups, outer, 0)

    z_ref[...] = jnp.zeros((vrows, LANES), F32)

    def step(opening, n, carry):
        c = n & (COLORS - 1)
        cf = c.astype(F32)
        if opening:
            same_field(c, ((v_ref, tv_ref), (den_ref, td_ref)))
            for k in range(groups):
                rows = slice(k * pair, (k + 1) * pair)
                den_ref[rows] = jnp.where(col_ref[rows] == cf, 1.0 / (td_ref[rows] + PRIOR_WEIGHT), den_ref[rows])
        else:
            same_field(c, ((v_ref, tv_ref),))
        for k in range(groups):
            rows = slice(k * pair, (k + 1) * pair)
            old = z_ref[rows]
            new = jnp.where(col_ref[rows] == cf, tv_ref[rows] * den_ref[rows], old)
            z_ref[rows] = new
            diff = new - old
            turned = pltpu.roll(diff, HALF, 1)
            dz_ref[2 * k * pair : (2 * k + 1) * pair, :] = jnp.where(low8, diff, turned)
            dz_ref[(2 * k + 1) * pair : (2 * k + 2) * pair, :] = jnp.where(low8, turned, diff)

        def apply(q, accs):
            first = q * (2 * bands)
            rows = [row_to(dz_ref[pl.ds(first + i, 1), :], pair) for i in range(2 * bands)]
            out = []
            for k in range(groups):
                terms = []
                for i in range(2 * bands):
                    gram_ref, kk = (ga_ref, k) if k < groups // 2 else (gb_ref, k - groups // 2)
                    base = pl.multiple_of((first + i) * (vrows // 2) + kk * pair, pair)
                    terms.append(gram_ref[pl.ds(base, pair), :] * rows[i])
                while len(terms) > 1:
                    terms = [terms[i] + terms[i + 1] for i in range(0, len(terms), 2)]
                out.append(accs[k] + terms[0])
            return tuple(out)

        start = tuple(v_ref[k * pair : (k + 1) * pair] for k in range(groups))
        done = lax.fori_loop(lim_ref[0, c] >> 1, (lim_ref[1, c] + 1) >> 1, apply, start)
        for k in range(groups):
            v_ref[k * pair : (k + 1) * pair, :] = done[k]

        @pl.when(c == COLORS - 1)
        def keep():
            zs_ref[n >> (COLORS.bit_length() - 1)] = z_ref[...]

        return carry

    lax.fori_loop(0, COLORS, functools.partial(step, True), 0)
    lax.fori_loop(COLORS, SWEEPS * COLORS, functools.partial(step, False), 0)

    tab = keep_ref[base_row : base_row + SUBS, stars : stars + LANES].astype(I32)
    low = base_row + SUBS
    mix_ref = [keep_ref[low : low + 1, (span + b) * LANES : (span + b + 1) * LANES] for b in range(bands)]
    for i in range(span):
        rk_ref[i * SUBS : (i + 1) * SUBS, :] = keep_ref[low : low + SUBS, i * LANES : (i + 1) * LANES]
    for sweep in range(SWEEPS):
        sq_ref[...] = jnp.zeros((LANES, LANES), F32)
        sq_ref[0:vrows, :] = zs_ref[sweep]
        et_ref[...] = sq_ref[...].T
        first = et_ref[0:SUBS, :]
        second = et_ref[HALF : HALF + SUBS, :]
        table = jnp.where(low8, first, pltpu.roll(second, HALF, 1))
        for b in range(bands):
            ze_ref[sweep * bands + b] = pick(table, tab + b)

    squares = [jnp.zeros((obs, LANES), F32) for _ in range(SWEEPS)]
    for chunk in range(stars // LANES):
        at = slice(chunk * LANES, (chunk + 1) * LANES)
        blk = chunk * LANES // blk_rows
        pred = [jnp.zeros((1, LANES), F32) for _ in range(SWEEPS)]
        own_mean = jnp.zeros((1, LANES), F32)
        for b in range(bands):
            w = keep_ref[2 * obs * b : 2 * obs * b + obs, at]
            slot = keep_ref[2 * obs * b + obs : 2 * obs * (b + 1), at].astype(I32)
            inverse = 1.0 / jnp.sum(w, axis=0, keepdims=True)
            base = keep_ref[2 * obs * b + chunk : 2 * obs * b + chunk + 1, stars : stars + LANES]
            for sweep in range(SWEEPS):
                seen = pick(row_to(ze_ref[sweep * bands + b, blk : blk + 1, :], obs), slot)
                mean = base - jnp.sum(w * seen, axis=0, keepdims=True) * inverse
                pred[sweep] = pred[sweep] + mix_ref[b] * mean
                if sweep == SWEEPS - 1:
                    own_mean = jnp.where(mine == b, mean, own_mean)
        means_ref[0:1, at] = own_mean
        first = pl.multiple_of(mine * (2 * obs), SUBS)
        w = keep_ref[pl.ds(first, obs), at]
        slot = keep_ref[pl.ds(first + obs, obs), at].astype(I32)
        mag = keep_ref[base_row : base_row + SUBS, at]
        for sweep in range(SWEEPS):
            seen = pick(row_to(ze_ref[sweep * bands + mine, blk : blk + 1, :], obs), slot)
            gap = mag - pred[sweep] - seen
            squares[sweep] = squares[sweep] + w * gap * gap
    result = jnp.zeros((1, LANES), F32)
    for sweep in range(SWEEPS):
        result = jnp.where(lane8[0:1] == sweep, jnp.sum(squares[sweep]), result)
    misfit_ref[...] = result

    frows = fields // LANES
    ids = jnp.where(fld2 < 0.0, 0.0, fld2).astype(I32)
    ranks = jnp.where(fld2 < 0.0, -1.0, table_lookup(rk_ref, ids, frows, -1.0))
    sq_ref[...] = jnp.full((LANES, LANES), -1.0, F32)
    sq_ref[0:srows, :] = ranks
    columns = sq_ref[...].T
    hi, mid, lo = split3(z_ref[pl.ds(mine, srows, stride=bands), :])
    places = iota((LANES, owned), 1).astype(F32)
    ones = jnp.ones((1, LANES), F32)
    total = jnp.zeros((SUBS, owned), F32)
    for r in range(srows):
        one_hot = jnp.where(jnp.broadcast_to(columns[:, r : r + 1], (LANES, owned)) == places, 1.0, 0.0)
        lhs = jnp.concatenate([hi[r : r + 1], mid[r : r + 1], lo[r : r + 1], ones, jnp.zeros((4, LANES), F32)], axis=0)
        total = total + lax.dot_general(lhs.astype(BF16), one_hot.astype(BF16), NN, preferred_element_type=F32)
    zp_ref[...] = (total[0:1] + (total[1:2] + total[2:3])) / jnp.maximum(total[3:4], 1.0)


def vmem():
    return pl.BlockSpec(memory_space=pltpu.VMEM)


def smem():
    return pl.BlockSpec(memory_space=pltpu.SMEM)


def move(value, bands, tiles, where):
    pairs = []
    for tile in range(tiles):
        for band in range(bands):
            z, y, x, c = where(tile >> 1, tile & 1, band >> 1, band & 1)
            pairs.append((tile * bands + band, (z * 2 + y) * bands + x * 2 + c))
    return lax.ppermute(value, ("sky", "band"), pairs)


def replicate(halves, bands, tiles):
    layers = tiles // 2
    send = lambda value, where: move(value, bands, tiles, where)
    order = sorted(range(1, layers), key=lambda k: -min(k, layers - k))
    other = lambda z, y, x, c: (z, y, x, c ^ 1)
    spread = []
    for half in halves:
        got = {k: send(half, lambda z, y, x, c, k=k: ((z + k) % layers, y, x, c)) for k in order}
        line = jnp.stack([half] + [got[k] for k in range(1, layers)])
        beside = send(line, lambda z, y, x, c: (z, y ^ 1, x, c) if c == 0 else (z, y, x ^ 1, c))
        near = jnp.concatenate([line, beside])
        across = send(near, lambda z, y, x, c: (z, y, x ^ 1, c) if c == 0 else (z, y ^ 1, x, c))
        spread.append([near, across, send(near, other), send(across, other)])
    return spread


def sky_sum(value, bands, tiles):
    value = value + move(value, bands, tiles, lambda z, y, x, c: (z, y ^ 1, x, c))
    step = 1
    while step < tiles // 2:
        value = value + move(value, bands, tiles, lambda z, y, x, c, s=step: (z ^ s, y, x, c))
        step *= 2
    return value


def local_body(magnitudes, weights, slots, block_fields, owner, colors, color_terms):
    bands = color_terms.shape[0]
    tiles = lax.axis_size("sky")
    _, obs, stars = magnitudes.shape
    blocks, entries = block_fields.shape
    fields = owner.shape[0]
    blk_rows = stars // blocks
    owned = fields // tiles
    mags, wts, slt = magnitudes[0], weights[0], slots[0]
    packed = pl.pallas_call(
        pack_kernel,
        name="pack",
        out_shape=jax.ShapeDtypeStruct((2 * obs, stars + LANES), F32),
        in_specs=[vmem()] * 3,
        out_specs=vmem(),
    )(mags, wts, slt)
    raw = lax.all_gather(packed, "band", axis=0)

    rows_half = entries * SUBS // 2
    first, second, tab = pl.pallas_call(
        functools.partial(tile_kernel, (bands, obs, stars, blocks, entries, fields, blk_rows)),
        name="tile",
        out_shape=(
            jax.ShapeDtypeStruct((rows_half + SUBS, LANES), F32),
            jax.ShapeDtypeStruct((rows_half + 2 * SUBS, LANES), F32),
            jax.ShapeDtypeStruct((SUBS, LANES), I32),
        ),
        in_specs=[smem(), vmem(), vmem(), vmem(), vmem()],
        out_specs=(vmem(), vmem(), vmem()),
        scratch_shapes=[
            pltpu.VMEM((SUBS, LANES), I32),
            pltpu.VMEM((LANES, LANES), F32),
            pltpu.VMEM((bands * entries, blk_rows), F32),
            pltpu.VMEM((bands * entries, blk_rows), F32),
            pltpu.VMEM((fields // LANES, LANES), F32),
        ],
    )(color_terms, raw, mags, block_fields, colors.reshape(-1, LANES))

    late, early = replicate((second, first), bands, tiles)
    groups = entries // 4
    pair = 2 * bands
    vrows = groups * pair
    state = jax.ShapeDtypeStruct((vrows, LANES), F32)
    square = pltpu.VMEM((LANES, LANES), F32)
    rows_state = pltpu.VMEM((vrows, LANES), F32)
    *ready, limits = pl.pallas_call(
        functools.partial(ready_kernel, (tiles, bands, entries)),
        name="ready",
        out_shape=(
            state,
            state,
            state,
            state,
            jax.ShapeDtypeStruct((bands * entries * vrows // 2, LANES), F32),
            jax.ShapeDtypeStruct((COLORS * MOST, 2 * LANES, 2 * LANES), BF16),
            jax.ShapeDtypeStruct((3, COLORS), I32),
        ),
        in_specs=[vmem()] * 4,
        out_specs=(vmem(),) * 6 + (smem(),),
        scratch_shapes=[square, square],
        compiler_params=pltpu.CompilerParams(vmem_limit_bytes=20 * 1024 * 1024),
    )(*early)
    keep = pl.pallas_call(
        functools.partial(side_kernel, (bands, fields, stars)),
        name="side",
        out_shape=jax.ShapeDtypeStruct((2 * obs * bands + 2 * SUBS, stars + LANES), F32),
        in_specs=[smem()] + [vmem()] * 4,
        out_specs=vmem(),
    )(color_terms, owner.reshape(-1, LANES), raw, mags, tab)

    zp, means, partial = pl.pallas_call(
        functools.partial(sweep_kernel, (tiles, bands, obs, stars, blocks, entries, fields, blk_rows, owned)),
        name="sweeps",
        out_shape=(
            jax.ShapeDtypeStruct((1, owned), F32),
            jax.ShapeDtypeStruct((1, stars), F32),
            jax.ShapeDtypeStruct((1, LANES), F32),
        ),
        in_specs=[smem()] + [vmem()] * 11,
        out_specs=(vmem(), vmem(), vmem()),
        scratch_shapes=[
            square,
            rows_state,
            rows_state,
            pltpu.VMEM((bands * entries * vrows // 2, LANES), F32),
            rows_state,
            pltpu.VMEM((bands * entries, LANES), F32),
            pltpu.VMEM((SWEEPS, vrows, LANES), F32),
            square,
            pltpu.VMEM((2 * groups, LANES, LANES), F32),
            pltpu.VMEM((2 * groups, SUBS, LANES), F32),
            rows_state,
            pltpu.VMEM((SWEEPS * bands, SUBS, LANES), F32),
            pltpu.VMEM((groups, 4 * bands, 2 * LANES), F32),
            rows_state,
            pltpu.VMEM((fields // LANES, LANES), F32),
        ],
        compiler_params=pltpu.CompilerParams(vmem_limit_bytes=20 * 1024 * 1024),
    )(limits, *late, *ready, keep)

    misfit = sky_sum(partial, bands, tiles)[0, :SWEEPS] / (obs * stars * tiles)
    return zp, means, misfit[:, None]


def fits_local(mesh, blocks_all, entries, stars, obs, bands, fields):
    tiles = mesh.shape["sky"]
    blocks = blocks_all // tiles
    return (
        2 * blocks_all == LANES
        and blocks == SUBS
        and bands == 4
        and bands * entries == LANES
        and obs == SUBS
        and 2 * bands == SUBS
        and mesh.shape["band"] == bands
        and stars // tiles == 2 * obs * LANES
        and (stars // blocks_all) % LANES == 0
        and fields % (SUBS * LANES) == 0
        and fields % (tiles * LANES) == 0
        and fields // SUBS + bands * LANES <= stars // tiles
    )


def from_behind(value, axis, steps):
    count = lax.axis_size(axis)
    pairs = [(source, (source + steps) % count) for source in range(count)]
    return lax.ppermute(value, axis, pairs)


def wide_body(magnitudes, weights, slots, block_fields, owner, colors, color_terms):
    band_count = color_terms.shape[0]
    tiles = lax.axis_size("sky")
    my_tile = lax.axis_index("sky")
    my_band = lax.axis_index("band")
    band_mags, band_wts, band_slots = (magnitudes, weights, slots)
    own_row = 0
    band_rows, obs_count, star_count = band_mags.shape
    block_count, list_len = block_fields.shape
    block_rows = star_count // block_count
    fields = owner.shape[0]
    slot_grid = band_slots.reshape(band_rows, obs_count, block_count, block_rows)
    entries = jnp.arange(list_len, dtype=jnp.int32)
    star_weight = jnp.sum(band_wts, axis=1)
    mixing = (
        jnp.eye(band_count, dtype=jnp.float32)
        + color_terms
        - jnp.diag(jnp.sum(color_terms, axis=1))
    )
    owner_order = jnp.argsort(owner, stable=True)
    owned = fields // tiles

    def slot_sums(values):
        grid = values.reshape(band_rows, obs_count, block_count, block_rows)
        hits = slot_grid[..., None] == entries
        return jnp.sum(jnp.where(hits, grid[..., None], 0.0), axis=(1, 3))

    def spread(list_vals):
        hits = slot_grid[..., None] == entries
        picked = jnp.sum(jnp.where(hits, list_vals[:, None, :, None, :], 0.0), axis=4)
        return picked.reshape(band_rows, obs_count, star_count)

    def predict(zp_obs):
        star_means = jnp.sum(band_wts * (band_mags - zp_obs), axis=1) / star_weight
        all_means = lax.all_gather(star_means, "band", axis=0, tiled=True)
        mix_row = lax.dynamic_index_in_dim(mixing, my_band, 0, keepdims=True)
        predicted = jnp.dot(mix_row, all_means, precision=lax.Precision.HIGHEST)
        return (star_means, predicted)

    positions = jnp.argsort(owner_order, stable=True)
    rank_in = positions - owner * owned
    live = block_fields < fields
    safe_ids = jnp.minimum(block_fields, fields - 1)
    relative = jnp.mod(jnp.take(owner, safe_ids) - my_tile + 1, tiles)
    list_ids = jnp.where(live, relative * owned + jnp.take(rank_in, safe_ids), 3 * owned)
    segments = 3 * owned
    nearby_idx = jnp.mod(my_tile + jnp.arange(3, dtype=jnp.int32) - 1, tiles)
    near_fields = jnp.take(owner_order.reshape(tiles, owned), nearby_idx, axis=0)
    zp_colors = jnp.take(colors, near_fields)[None]
    zero_pts = jnp.zeros((band_rows, 3, owned), jnp.float32)

    def flatten(table):
        return table.reshape(band_rows, 3 * owned)

    def combine(partial_flat):
        partial_sums = partial_flat.reshape(band_rows, 3, owned)
        from_left = from_behind(partial_sums[:, 1:3], "sky", 1)
        from_right = from_behind(partial_sums[:, 0:2], "sky", -1)
        far_left = from_behind(partial_sums[:, 2], "sky", 2)
        far_right = from_behind(partial_sums[:, 0], "sky", -2)
        below = far_left + from_left[:, 0] + partial_sums[:, 0]
        middle = from_left[:, 1] + partial_sums[:, 1] + from_right[:, 0]
        above = partial_sums[:, 2] + from_right[:, 1] + far_right
        return jnp.stack([below, middle, above], axis=1)

    def lookup(table):
        padded = jnp.concatenate([flatten(table), jnp.zeros((band_rows, 1), jnp.float32)], axis=1)
        return spread(jnp.take(padded, list_ids, axis=1))

    def segment_band(per_band):
        return jax.ops.segment_sum(
            per_band.reshape(-1), list_ids.reshape(-1), num_segments=segments + 1
        )[:segments]

    def totals(values):
        per_slot = slot_sums(values)
        return combine(jax.vmap(segment_band)(per_slot))

    denominators = totals(band_wts) + PRIOR_WEIGHT

    def squared_misfit(residual, zp_obs):
        per_band = jnp.sum(band_wts * (residual - zp_obs) ** 2, axis=(1, 2))
        return lax.dynamic_index_in_dim(per_band, own_row, 0, keepdims=False)

    def advance(table, color_no):
        zp_obs = lookup(table)
        _, predicted = predict(zp_obs)
        residual = band_mags - predicted[:, None, :]
        updated = totals(band_wts * residual) / denominators
        local_value = squared_misfit(residual, zp_obs)
        return (jnp.where(zp_colors == color_no, updated, table), local_value)

    def later_colors(color_no, table):
        return advance(table, color_no)[0]

    def record(local_value):
        return lax.psum(local_value, "sky")

    recorded = []
    for sweep_no in range(SWEEPS):
        zero_pts, local_value = advance(zero_pts, 0)
        if sweep_no > 0:
            recorded.append(record(local_value))
        zero_pts = lax.fori_loop(1, COLORS, later_colors, zero_pts)
    zp_obs = lookup(zero_pts)
    star_means, predicted = predict(zp_obs)
    residual = band_mags - predicted[:, None, :]
    recorded.append(record(squared_misfit(residual, zp_obs)))
    stacked = jnp.stack(recorded)
    misfit = stacked / (obs_count * star_count * tiles)
    own_zp = lax.dynamic_index_in_dim(zero_pts[:, 1], own_row, 0, keepdims=True)
    own_means = lax.dynamic_index_in_dim(star_means, own_row, 0, keepdims=True)
    return (own_zp, own_means, misfit[:, None])


def solution(mesh):
    in_specs = (
        P("band", None, "sky"),
        P("band", None, "sky"),
        P("band", None, "sky"),
        P("sky", None),
        P(),
        P(),
        P(),
    )
    out_specs = (P("band", "sky"), P("band", "sky"), P(None, "band"))

    def call(magnitudes, weights, slots, block_fields, owner, colors, color_terms):
        bands, obs, stars = magnitudes.shape
        blocks_all, entries = block_fields.shape
        local = fits_local(mesh, blocks_all, entries, stars, obs, bands, owner.shape[0])
        body = local_body if local else wide_body
        run = jax.shard_map(body, mesh=mesh, in_specs=in_specs, out_specs=out_specs, check_vma=False)
        return run(magnitudes, weights, slots, block_fields, owner, colors, color_terms)

    return call
```

```python
import functools

import jax
import jax.numpy as jnp
from jax import lax
from jax.experimental import pallas as pl
from jax.experimental.pallas import tpu as pltpu
from jax.sharding import PartitionSpec as P


COLORS = 8
SWEEPS = 4


PRIOR_WEIGHT = 1.0
LANES = 128
SUBS = 8
HALF = LANES // 2
FOLDS = (2, 3)
MOST = max(FOLDS) ** 2
F32 = jnp.float32
BF16 = jnp.bfloat16
I32 = jnp.int32
NT = (((1,), (1,)), ((), ()))
NN = (((1,), (0,)), ((), ()))


def iota(shape, axis):
    return lax.broadcasted_iota(I32, shape, axis)


def pick(table, idx):
    return jnp.take_along_axis(table, idx, axis=1, mode="promise_in_bounds")


def row_to(value, rows):
    return jnp.broadcast_to(value, (rows, value.shape[1]))


def table_lookup(table_ref, ids, rows, init):
    out = jnp.full(ids.shape, init, F32)
    for r in range(rows):
        hit = pick(row_to(table_ref[r : r + 1, :], ids.shape[0]), ids & (LANES - 1))
        out = jnp.where((ids >> 7) == r, hit, out)
    return out


def mixing_row(terms_ref, mine, bands):
    total = terms_ref[mine, 0]
    for b in range(1, bands):
        total = total + terms_ref[mine, b]
    return [terms_ref[mine, b] + jnp.where(mine == b, 1.0 - total, 0.0) for b in range(bands)]


def pack_kernel(mag_ref, wt_ref, slot_ref, out_ref):
    obs, stars = mag_ref.shape
    w = wt_ref[...]
    out_ref[0:obs, 0:stars] = w
    out_ref[obs : 2 * obs, 0:stars] = slot_ref[...].astype(F32)
    base = jnp.sum(w * mag_ref[...], axis=0, keepdims=True) / jnp.sum(w, axis=0, keepdims=True)
    for i in range(stars // LANES):
        out_ref[i : i + 1, stars : stars + LANES] = base[:, i * LANES : (i + 1) * LANES]


def tile_kernel(
    dims, terms_ref, raw_ref, mag_ref, lists_ref, colors_ref, out0_ref, out1_ref, tab_ref, pad_ref, sq_ref, wf_ref, x_ref, colf_ref
):
    bands, obs, stars, blocks, entries, fields, blk_rows = dims
    lane = iota((SUBS, LANES), 1)
    pad_ref[...] = jnp.full((SUBS, LANES), fields, I32)
    pad_ref[:, :entries] = lists_ref[...]
    ids = pad_ref[...]
    live = ids < fields
    safe = jnp.where(live, ids, 0)
    colf_ref[...] = colors_ref[...].astype(F32)
    color = table_lookup(colf_ref, safe, fields // LANES, 0.0).astype(I32)
    key = jnp.where(live, color * entries + lane, COLORS * entries)
    rank = jnp.zeros((SUBS, LANES), I32)
    for e in range(entries):
        rank = rank + jnp.where(key[:, e : e + 1] < key, 1, 0)
    live_f = jnp.where(live, 1.0, 0.0)
    dead = entries - jnp.sum(live_f, axis=1, keepdims=True).astype(I32)
    pos = jnp.where(live, rank + ((dead * color) >> (COLORS.bit_length() - 1)), 4 * LANES)
    inv = jnp.full((SUBS, LANES), -1, I32)
    for e in range(entries):
        inv = jnp.where(pos[:, e : e + 1] == lane, e, inv)
    used = inv >= 0
    inv_safe = jnp.where(used, inv, 0)
    fpos = jnp.where(used, pick(ids, inv_safe).astype(F32), -1.0)
    cpos = jnp.where(used, pick(color, inv_safe).astype(F32), float(COLORS))
    pos_live = jnp.where(live, pos, 0)
    tab_ref[...] = ((pos_live >> 1) & 1) * HALF + (pos_live >> 2) * (2 * bands) + (pos_live & 1) * bands

    sq_ref[...] = jnp.zeros((LANES, LANES), F32)
    sq_ref[0:SUBS, :] = inv.astype(F32)
    inv_t = sq_ref[...].T
    mine = lax.axis_index("band")
    mix_ref = mixing_row(terms_ref, mine, bands)
    lanes_sq = iota((entries, LANES), 1)
    t0_cols = jnp.zeros((entries, LANES), F32)
    wt_cols = jnp.zeros((entries, LANES), F32)
    for blk in range(blocks):
        lo, hi = blk * blk_rows, (blk + 1) * blk_rows
        inv_col = jnp.broadcast_to(inv_t[0:entries, blk : blk + 1], (entries, blk_rows))
        pred = jnp.zeros((1, blk_rows), F32)
        for b in range(bands):
            w = raw_ref[b, 0:obs, lo:hi]
            slot = raw_ref[b, obs : 2 * obs, lo:hi]
            acc = jnp.zeros((entries, blk_rows), F32)
            for k in range(obs):
                acc = acc + jnp.where(slot[k : k + 1] == inv_col, w[k : k + 1], 0.0)
            scale = mix_ref[b] / jnp.sum(w, axis=0, keepdims=True)
            wf_ref[b * entries : (b + 1) * entries, :] = acc
            x_ref[b * entries : (b + 1) * entries, :] = acc * scale
            pieces = blk_rows // LANES
            means = raw_ref[b, blk * pieces : (blk + 1) * pieces, stars : stars + LANES]
            pred = pred + mix_ref[b] * jnp.concatenate([means[i : i + 1] for i in range(pieces)], axis=1)
        own = wf_ref[pl.ds(mine * entries, entries), :]
        gram = lax.dot_general(own, x_ref[...], NT, precision=lax.Precision.HIGHEST, preferred_element_type=F32)
        cut = entries // 2
        out0_ref[pl.ds(SUBS + blk, cut, stride=SUBS), :] = gram[:cut]
        out1_ref[pl.ds(blk, cut, stride=SUBS), :] = gram[cut:]
        w = raw_ref[mine, 0:obs, lo:hi]
        slot = raw_ref[mine, obs : 2 * obs, lo:hi]
        value = w * (mag_ref[:, lo:hi] - pred)
        acc = jnp.zeros((entries, blk_rows), F32)
        for k in range(obs):
            acc = acc + jnp.where(slot[k : k + 1] == inv_col, value[k : k + 1], 0.0)
        t0_cols = jnp.where(lanes_sq == blk, jnp.sum(acc, axis=1, keepdims=True), t0_cols)
        wt_cols = jnp.where(lanes_sq == blk, jnp.sum(own, axis=1, keepdims=True), wt_cols)
    sq_ref[...] = jnp.zeros((LANES, LANES), F32)
    sq_ref[0:entries, :] = t0_cols
    sq_ref[entries : 2 * entries, :] = wt_cols
    flipped = sq_ref[...].T[0:SUBS]
    extra = jnp.where(lane < 3 * entries, pltpu.roll(fpos, 2 * entries, 1), pltpu.roll(cpos, 3 * entries, 1))
    out1_ref[entries * SUBS // 2 :, :] = jnp.zeros((2 * SUBS, LANES), F32)
    out0_ref[0:SUBS, :] = jnp.where(lane < 2 * entries, flipped, extra)


def split3(value):
    hi = value.astype(BF16).astype(F32)
    rest = value - hi
    mid = rest.astype(BF16).astype(F32)
    return hi, mid, rest - mid


def tile_order(tiles):
    return [(dy, back) for dy in range(2) for back in range(tiles // 2)]


def gathered(part, swap, layers, dc, dx, dy, back, rows):
    d1, d2 = (dx, dy) if (dc == 1) != swap else (dy, dx)
    return part[2 * dc + d2][d1 * layers + back, rows, :]


def by_core(mine, run):
    pl.when((mine & 1) == 0)(functools.partial(run, False))
    pl.when((mine & 1) != 0)(functools.partial(run, True))


def turn_half(part, swap, mine, tiles, bands, entries, skip, dest_ref):
    groups = entries // 8
    pair = 2 * bands
    vrows = groups * pair

    def turn(k, carry):
        for p in range(2):
            for dx in range(2):
                for dc in range(2):
                    b = ((mine >> 1) ^ dx) * 2 + ((mine & 1) ^ dc)
                    rows = []
                    for half in range(2):
                        start = pl.multiple_of((4 * k + 2 * half + p) * SUBS + skip, SUBS)
                        for dy, back in tile_order(tiles):
                            rows.append(gathered(part, swap, tiles // 2, dc, dx, dy, back, pl.ds(start, SUBS)))
                    flipped = jnp.concatenate(rows, axis=0).T
                    for b2 in range(bands):
                        at = pl.ds(b2 * vrows + k * pair + p * bands + b, entries, stride=bands * vrows)
                        dest_ref[at, :] = flipped[b2 * entries : (b2 + 1) * entries]
        return carry

    lax.fori_loop(0, groups, turn, 0)


def fold_of(lim_ref, c):
    most = lim_ref[2, c]
    bounds = [0] + [4 * fold for fold in FOLDS]
    return [(fold, (most > low) & (most <= high)) for fold, low, high in zip(FOLDS, bounds, bounds[1:])], most > bounds[-1]


def side_kernel(dims, terms_ref, owner_ref, raw_in, mag_in, tab_in, keep_ref):
    bands, fields, stars = dims
    raw_rows = raw_in.shape[1]
    base = bands * raw_rows
    for b in range(bands):
        keep_ref[b * raw_rows : (b + 1) * raw_rows, :] = raw_in[b]
    keep_ref[base : base + SUBS, 0:stars] = mag_in[...]
    keep_ref[base : base + SUBS, stars : stars + LANES] = tab_in[...].astype(F32)
    low = base + SUBS
    span = fields // LANES // SUBS
    for b, value in enumerate(mixing_row(terms_ref, lax.axis_index("band"), bands)):
        keep_ref[low : low + SUBS, (span + b) * LANES : (span + b + 1) * LANES] = jnp.full((SUBS, LANES), value, F32)
    my_tile = lax.axis_index("sky")
    frows = fields // LANES
    own = jnp.where(owner_ref[...] == my_tile, 1.0, 0.0)
    upto = jnp.where(iota((LANES, LANES), 0) <= iota((LANES, LANES), 1), 1.0, 0.0).astype(BF16)
    inside = lax.dot_general(own.astype(BF16), upto, NN, preferred_element_type=F32)
    sums = jnp.broadcast_to(jnp.sum(own, axis=1, keepdims=True), (frows, LANES))
    before = jnp.where(iota((frows, frows), 1) < iota((frows, frows), 0), 1.0, 0.0).astype(BF16)
    ahead = lax.dot_general(before, sums.astype(BF16), NN, preferred_element_type=F32)
    ranks = jnp.where(own > 0.0, inside + ahead - 1.0, -1.0)
    for i in range(span):
        keep_ref[low : low + SUBS, i * LANES : (i + 1) * LANES] = ranks[i * SUBS : (i + 1) * SUBS]


def fields_kernel(dims, near_ref, far_near_ref, s_ref, lim_ref, sq_ref, et_ref, fld_ref, col_ref):
    tiles, entries = dims
    groups = entries // 4
    low8 = iota((SUBS, LANES), 1) < HALF
    mine = lax.axis_index("band")

    def load(swap):
        source = far_near_ref if swap else near_ref
        sq_ref[...] = jnp.zeros((LANES, LANES), F32)
        for t in range(tiles):
            sq_ref[t * SUBS : (t + 1) * SUBS, :] = source[t, 0:SUBS, :]
        et_ref[...] = sq_ref[...].T
        for p in range(2):
            for q, dest in ((2, fld_ref), (3, col_ref)):
                first = et_ref[pl.ds(q * entries + p, groups, stride=4), :]
                second = et_ref[pl.ds(q * entries + 2 + p, groups, stride=4), :]
                dest[pl.ds(p, groups, stride=2), :] = jnp.where(low8, first, pltpu.roll(second, HALF, 1))

    by_core(mine, load)
    srows = 2 * groups
    fld2 = fld_ref[...]
    col2 = col_ref[...]
    row2 = iota((srows, LANES), 0)
    position = 4 * (row2 >> 1) + 2 * jnp.where(iota((srows, LANES), 1) < HALF, 0, 1) + (row2 & 1)
    for c in range(COLORS):
        hit = col2 == float(c)
        lim_ref[0, c] = jnp.min(jnp.where(hit, position, entries))
        lim_ref[1, c] = jnp.max(jnp.where(hit, position + 1, 0))
        count = jnp.sum(jnp.where(hit, 1.0, 0.0), axis=0, keepdims=True)
        lim_ref[2, c] = jnp.max(count + pltpu.roll(count, HALF, 1)).astype(I32)

    def build_fold(c, fold):
        chosen = jnp.where(col2 == c.astype(F32), fld2, -1.0)
        folded = []
        for m in range(fold):
            for p in range(2):
                best = jnp.full((1, LANES), -1.0, F32)
                for k in range(m, groups, fold):
                    best = jnp.maximum(best, chosen[2 * k + p : 2 * k + p + 1])
                folded.append(best)
        sq_ref[0 : 2 * fold, :] = jnp.concatenate(folded, axis=0)
        columns = sq_ref[...].T
        others = [jnp.where(row < 0.0, -2.0, row) for row in folded]
        for i in range(2 * fold):
            col = jnp.broadcast_to(columns[:, i : i + 1], (LANES, LANES))
            for j in range(2 * fold):
                tile = jnp.where(col == others[j], 1.0, 0.0).astype(BF16)
                m, p, n, r = i // 2, i % 2, j // 2, j % 2
                s_ref[c * MOST + m * fold + n, p * LANES : (p + 1) * LANES, r * LANES : (r + 1) * LANES] = tile

    def build(c, carry):
        for fold, chosen in fold_of(lim_ref, c)[0]:
            pl.when(chosen)(functools.partial(build_fold, c, fold))
        return carry

    lax.fori_loop(0, COLORS, build, 0)


def ready_kernel(
    dims, near_ref, across_ref, far_near_ref, far_across_ref,
    v_ref, den_ref, fld_ref, col_ref, g_ref, sq_ref, et_ref,
):
    tiles, bands, entries = dims
    groups = entries // 4
    pair = 2 * bands
    low8 = iota((SUBS, LANES), 1) < HALF
    mine = lax.axis_index("band")
    part = (near_ref, across_ref, far_near_ref, far_across_ref)

    def load(swap):
        for dx in range(2):
            for dc in range(2):
                b = ((mine >> 1) ^ dx) * 2 + ((mine & 1) ^ dc)
                sq_ref[...] = jnp.zeros((LANES, LANES), F32)
                for t, (dy, back) in enumerate(tile_order(tiles)):
                    sq_ref[t * SUBS : (t + 1) * SUBS, :] = gathered(
                        part, swap, tiles // 2, dc, dx, dy, back, slice(0, SUBS)
                    )
                et_ref[...] = sq_ref[...].T
                for p in range(2):
                    for q, dest in enumerate((v_ref, den_ref, fld_ref, col_ref)):
                        first = et_ref[pl.ds(q * entries + p, groups, stride=4), :]
                        second = et_ref[pl.ds(q * entries + 2 + p, groups, stride=4), :]
                        dest[pl.ds(p * bands + b, groups, stride=pair), :] = jnp.where(
                            low8, first, pltpu.roll(second, HALF, 1)
                        )
        turn_half(part, swap, mine, tiles, bands, entries, SUBS, g_ref)

    by_core(mine, load)


def sweep_kernel(
    dims, lim_ref, near_ref, across_ref, far_near_ref, far_across_ref,
    v0_ref, wsum_ref, fld_ref, col_ref, ga_ref, s_ref, keep_ref,
    zp_ref, means_ref, misfit_ref,
    et_ref, v_ref, den_ref, gb_ref, z_ref, dz_ref, zs_ref,
    sq_ref, fc_ref, fr_ref, tv_ref, ze_ref, big_ref, td_ref, rk_ref,
):
    tiles, bands, obs, stars, _, entries, fields, blk_rows, owned = dims
    groups = entries // 4
    pair = 2 * bands
    vrows = groups * pair
    lane8 = iota((SUBS, LANES), 1)
    low8 = lane8 < HALF
    mine = lax.axis_index("band")
    base_row = 2 * obs * bands
    span = fields // LANES // SUBS
    part = (near_ref, across_ref, far_near_ref, far_across_ref)
    by_core(mine, lambda swap: turn_half(part, swap, mine, tiles, bands, entries, 0, gb_ref))
    v_ref[...] = v0_ref[...]
    den_ref[...] = wsum_ref[...]
    srows = 2 * groups
    fld2 = fld_ref[pl.ds(0, srows, stride=bands), :]
    col2 = col_ref[pl.ds(0, srows, stride=bands), :]

    def spread_rows(value):
        flat = jnp.concatenate([value[0:bands], value[bands:pair]], axis=1)
        hi, mid, lo = split3(flat)
        return jnp.concatenate([hi, mid, lo, jnp.zeros_like(hi)], axis=0).astype(BF16)

    def pack_rows(total):
        flat = total[0:bands] + (total[bands : 2 * bands] + total[2 * bands : 3 * bands])
        return jnp.concatenate([flat[:, :LANES], flat[:, LANES:]], axis=0)

    def same_field(c, work):
        cf = c.astype(F32)
        choices, rest = fold_of(lim_ref, c)

        def fast(fold):
            lhs = []
            for m in range(fold):
                rows_of = []
                for src, _ in work:
                    total = jnp.zeros((pair, LANES), F32)
                    for k in range(m, groups, fold):
                        rows = slice(k * pair, (k + 1) * pair)
                        total = total + jnp.where(col_ref[rows] == cf, src[rows], 0.0)
                    rows_of.append(spread_rows(total))
                lhs.append(jnp.concatenate(rows_of, axis=0))
            for n in range(fold):
                total = jnp.zeros((4 * bands * len(work), 2 * LANES), F32)
                for m in range(fold):
                    total = total + lax.dot_general(
                        lhs[m], s_ref[c * MOST + m * fold + n], NN, preferred_element_type=F32
                    )
                for i, (_, dest) in enumerate(work):
                    packed = pack_rows(total[4 * bands * i : 4 * bands * (i + 1)])
                    for k in range(n, groups, fold):
                        dest[k * pair : (k + 1) * pair, :] = packed

        for fold, chosen in choices:
            pl.when(chosen)(functools.partial(fast, fold))

        @pl.when(rest)
        def general():
            for src, dest in work:
                one_general(cf, src, dest)

    def one_general(cf, src, dest):
        chosen = jnp.where(col2 == cf, fld2, -1.0)
        sq_ref[...] = jnp.full((LANES, LANES), -1.0, F32)
        sq_ref[0:srows, :] = chosen
        columns = sq_ref[...].T
        for i in range(srows):
            fc_ref[i] = jnp.broadcast_to(columns[:, i : i + 1], (LANES, LANES))
            fr_ref[i] = row_to(jnp.where(chosen[i : i + 1] < 0.0, -2.0, chosen[i : i + 1]), SUBS)
        for m in range(groups):
            rows = slice(m * pair, (m + 1) * pair)
            big_ref[m] = spread_rows(jnp.where(col_ref[rows] == cf, src[rows], 0.0)).astype(F32)

        def outer(n, carry):
            def inner(m, total):
                parts = []
                for r in range(2):
                    row = fr_ref[2 * n + r][0:1]
                    upper = jnp.where(fc_ref[2 * m] == row, 1.0, 0.0)
                    lower = jnp.where(fc_ref[2 * m + 1] == row, 1.0, 0.0)
                    lhs = big_ref[m].astype(BF16)
                    parts.append(
                        lax.dot_general(lhs[:, :LANES], upper.astype(BF16), NN, preferred_element_type=F32)
                        + lax.dot_general(lhs[:, LANES:], lower.astype(BF16), NN, preferred_element_type=F32)
                    )
                return total + jnp.concatenate(parts, axis=1)

            total = lax.fori_loop(0, groups, inner, jnp.zeros((4 * bands, 2 * LANES), F32))
            dest[pl.ds(pl.multiple_of(n * pair, pair), pair), :] = pack_rows(total)
            return carry

        lax.fori_loop(0, groups, outer, 0)

    z_ref[...] = jnp.zeros((vrows, LANES), F32)

    def step(opening, n, carry):
        c = n & (COLORS - 1)
        cf = c.astype(F32)
        if opening:
            same_field(c, ((v_ref, tv_ref), (den_ref, td_ref)))
            for k in range(groups):
                rows = slice(k * pair, (k + 1) * pair)
                den_ref[rows] = jnp.where(col_ref[rows] == cf, 1.0 / (td_ref[rows] + PRIOR_WEIGHT), den_ref[rows])
        else:
            same_field(c, ((v_ref, tv_ref),))
        for k in range(groups):
            rows = slice(k * pair, (k + 1) * pair)
            old = z_ref[rows]
            new = jnp.where(col_ref[rows] == cf, tv_ref[rows] * den_ref[rows], old)
            z_ref[rows] = new
            diff = new - old
            turned = pltpu.roll(diff, HALF, 1)
            dz_ref[2 * k * pair : (2 * k + 1) * pair, :] = jnp.where(low8, diff, turned)
            dz_ref[(2 * k + 1) * pair : (2 * k + 2) * pair, :] = jnp.where(low8, turned, diff)

        def apply(q, accs):
            first = q * (2 * bands)
            rows = [row_to(dz_ref[pl.ds(first + i, 1), :], pair) for i in range(2 * bands)]
            out = []
            for k in range(groups):
                terms = []
                for i in range(2 * bands):
                    gram_ref, kk = (ga_ref, k) if k < groups // 2 else (gb_ref, k - groups // 2)
                    base = pl.multiple_of((first + i) * (vrows // 2) + kk * pair, pair)
                    terms.append(gram_ref[pl.ds(base, pair), :] * rows[i])
                while len(terms) > 1:
                    terms = [terms[i] + terms[i + 1] for i in range(0, len(terms), 2)]
                out.append(accs[k] + terms[0])
            return tuple(out)

        start = tuple(v_ref[k * pair : (k + 1) * pair] for k in range(groups))
        done = lax.fori_loop(lim_ref[0, c] >> 1, (lim_ref[1, c] + 1) >> 1, apply, start)
        for k in range(groups):
            v_ref[k * pair : (k + 1) * pair, :] = done[k]

        @pl.when(c == COLORS - 1)
        def keep():
            zs_ref[n >> (COLORS.bit_length() - 1)] = z_ref[...]

        return carry

    lax.fori_loop(0, COLORS, functools.partial(step, True), 0)
    lax.fori_loop(COLORS, SWEEPS * COLORS, functools.partial(step, False), 0)

    tab = keep_ref[base_row : base_row + SUBS, stars : stars + LANES].astype(I32)
    low = base_row + SUBS
    mix_ref = [keep_ref[low : low + 1, (span + b) * LANES : (span + b + 1) * LANES] for b in range(bands)]
    for i in range(span):
        rk_ref[i * SUBS : (i + 1) * SUBS, :] = keep_ref[low : low + SUBS, i * LANES : (i + 1) * LANES]
    for sweep in range(SWEEPS):
        sq_ref[...] = jnp.zeros((LANES, LANES), F32)
        sq_ref[0:vrows, :] = zs_ref[sweep]
        et_ref[...] = sq_ref[...].T
        first = et_ref[0:SUBS, :]
        second = et_ref[HALF : HALF + SUBS, :]
        table = jnp.where(low8, first, pltpu.roll(second, HALF, 1))
        for b in range(bands):
            ze_ref[sweep * bands + b] = pick(table, tab + b)

    squares = [jnp.zeros((obs, LANES), F32) for _ in range(SWEEPS)]
    for chunk in range(stars // LANES):
        at = slice(chunk * LANES, (chunk + 1) * LANES)
        blk = chunk * LANES // blk_rows
        pred = [jnp.zeros((1, LANES), F32) for _ in range(SWEEPS)]
        own_mean = jnp.zeros((1, LANES), F32)
        for b in range(bands):
            w = keep_ref[2 * obs * b : 2 * obs * b + obs, at]
            slot = keep_ref[2 * obs * b + obs : 2 * obs * (b + 1), at].astype(I32)
            inverse = 1.0 / jnp.sum(w, axis=0, keepdims=True)
            base = keep_ref[2 * obs * b + chunk : 2 * obs * b + chunk + 1, stars : stars + LANES]
            for sweep in range(SWEEPS):
                seen = pick(row_to(ze_ref[sweep * bands + b, blk : blk + 1, :], obs), slot)
                mean = base - jnp.sum(w * seen, axis=0, keepdims=True) * inverse
                pred[sweep] = pred[sweep] + mix_ref[b] * mean
                if sweep == SWEEPS - 1:
                    own_mean = jnp.where(mine == b, mean, own_mean)
        means_ref[0:1, at] = own_mean
        first = pl.multiple_of(mine * (2 * obs), SUBS)
        w = keep_ref[pl.ds(first, obs), at]
        slot = keep_ref[pl.ds(first + obs, obs), at].astype(I32)
        mag = keep_ref[base_row : base_row + SUBS, at]
        for sweep in range(SWEEPS):
            seen = pick(row_to(ze_ref[sweep * bands + mine, blk : blk + 1, :], obs), slot)
            gap = mag - pred[sweep] - seen
            squares[sweep] = squares[sweep] + w * gap * gap
    result = jnp.zeros((1, LANES), F32)
    for sweep in range(SWEEPS):
        result = jnp.where(lane8[0:1] == sweep, jnp.sum(squares[sweep]), result)
    misfit_ref[...] = result

    frows = fields // LANES
    ids = jnp.where(fld2 < 0.0, 0.0, fld2).astype(I32)
    ranks = jnp.where(fld2 < 0.0, -1.0, table_lookup(rk_ref, ids, frows, -1.0))
    sq_ref[...] = jnp.full((LANES, LANES), -1.0, F32)
    sq_ref[0:srows, :] = ranks
    columns = sq_ref[...].T
    hi, mid, lo = split3(z_ref[pl.ds(mine, srows, stride=bands), :])
    places = iota((LANES, owned), 1).astype(F32)
    ones = jnp.ones((1, LANES), F32)
    total = jnp.zeros((SUBS, owned), F32)
    for r in range(srows):
        one_hot = jnp.where(jnp.broadcast_to(columns[:, r : r + 1], (LANES, owned)) == places, 1.0, 0.0)
        lhs = jnp.concatenate([hi[r : r + 1], mid[r : r + 1], lo[r : r + 1], ones, jnp.zeros((4, LANES), F32)], axis=0)
        total = total + lax.dot_general(lhs.astype(BF16), one_hot.astype(BF16), NN, preferred_element_type=F32)
    zp_ref[...] = (total[0:1] + (total[1:2] + total[2:3])) / jnp.maximum(total[3:4], 1.0)


def vmem():
    return pl.BlockSpec(memory_space=pltpu.VMEM)


def smem():
    return pl.BlockSpec(memory_space=pltpu.SMEM)


def move(value, bands, tiles, where):
    pairs = []
    for tile in range(tiles):
        for band in range(bands):
            z, y, x, c = where(tile >> 1, tile & 1, band >> 1, band & 1)
            pairs.append((tile * bands + band, (z * 2 + y) * bands + x * 2 + c))
    return lax.ppermute(value, ("sky", "band"), pairs)


def replicate(halves, bands, tiles):
    layers = tiles // 2
    send = lambda value, where: move(value, bands, tiles, where)
    order = sorted(range(1, layers), key=lambda k: -min(k, layers - k))
    other = lambda z, y, x, c: (z, y, x, c ^ 1)
    spread = []
    for half in halves:
        got = {k: send(half, lambda z, y, x, c, k=k: ((z + k) % layers, y, x, c)) for k in order}
        line = jnp.stack([half] + [got[k] for k in range(1, layers)])
        beside = send(line, lambda z, y, x, c: (z, y ^ 1, x, c) if c == 0 else (z, y, x ^ 1, c))
        near = jnp.concatenate([line, beside])
        across = send(near, lambda z, y, x, c: (z, y, x ^ 1, c) if c == 0 else (z, y ^ 1, x, c))
        spread.append([near, across, send(near, other), send(across, other)])
    return spread


def sky_sum(value, bands, tiles):
    value = value + move(value, bands, tiles, lambda z, y, x, c: (z, y ^ 1, x, c))
    step = 1
    while step < tiles // 2:
        value = value + move(value, bands, tiles, lambda z, y, x, c, s=step: (z ^ s, y, x, c))
        step *= 2
    return value


def local_body(magnitudes, weights, slots, block_fields, owner, colors, color_terms):
    bands = color_terms.shape[0]
    tiles = lax.axis_size("sky")
    _, obs, stars = magnitudes.shape
    blocks, entries = block_fields.shape
    fields = owner.shape[0]
    blk_rows = stars // blocks
    owned = fields // tiles
    mags, wts, slt = magnitudes[0], weights[0], slots[0]
    packed = pl.pallas_call(
        pack_kernel,
        name="pack",
        out_shape=jax.ShapeDtypeStruct((2 * obs, stars + LANES), F32),
        in_specs=[vmem()] * 3,
        out_specs=vmem(),
    )(mags, wts, slt)
    raw = lax.all_gather(packed, "band", axis=0)

    rows_half = entries * SUBS // 2
    first, second, tab = pl.pallas_call(
        functools.partial(tile_kernel, (bands, obs, stars, blocks, entries, fields, blk_rows)),
        name="tile",
        out_shape=(
            jax.ShapeDtypeStruct((rows_half + SUBS, LANES), F32),
            jax.ShapeDtypeStruct((rows_half + 2 * SUBS, LANES), F32),
            jax.ShapeDtypeStruct((SUBS, LANES), I32),
        ),
        in_specs=[smem(), vmem(), vmem(), vmem(), vmem()],
        out_specs=(vmem(), vmem(), vmem()),
        scratch_shapes=[
            pltpu.VMEM((SUBS, LANES), I32),
            pltpu.VMEM((LANES, LANES), F32),
            pltpu.VMEM((bands * entries, blk_rows), F32),
            pltpu.VMEM((bands * entries, blk_rows), F32),
            pltpu.VMEM((fields // LANES, LANES), F32),
        ],
    )(color_terms, raw, mags, block_fields, colors.reshape(-1, LANES))

    late, early = replicate((second, first), bands, tiles)
    groups = entries // 4
    pair = 2 * bands
    vrows = groups * pair
    state = jax.ShapeDtypeStruct((vrows, LANES), F32)
    square = pltpu.VMEM((LANES, LANES), F32)
    rows_state = pltpu.VMEM((vrows, LANES), F32)
    ready = pl.pallas_call(
        functools.partial(ready_kernel, (tiles, bands, entries)),
        name="ready",
        out_shape=(state, state, state, state, jax.ShapeDtypeStruct((bands * entries * vrows // 2, LANES), F32)),
        in_specs=[vmem()] * 4,
        out_specs=(vmem(),) * 5,
        scratch_shapes=[square, square],
        compiler_params=pltpu.CompilerParams(vmem_limit_bytes=20 * 1024 * 1024),
    )(*early)
    same, limits = pl.pallas_call(
        functools.partial(fields_kernel, (tiles, entries)),
        name="fields",
        out_shape=(
            jax.ShapeDtypeStruct((COLORS * MOST, 2 * LANES, 2 * LANES), BF16),
            jax.ShapeDtypeStruct((3, COLORS), I32),
        ),
        in_specs=[vmem()] * 2,
        out_specs=(vmem(), smem()),
        scratch_shapes=[square, square] + [pltpu.VMEM((2 * groups, LANES), F32)] * 2,
        compiler_params=pltpu.CompilerParams(vmem_limit_bytes=20 * 1024 * 1024),
    )(early[0], early[2])
    keep = pl.pallas_call(
        functools.partial(side_kernel, (bands, fields, stars)),
        name="side",
        out_shape=jax.ShapeDtypeStruct((2 * obs * bands + 2 * SUBS, stars + LANES), F32),
        in_specs=[smem()] + [vmem()] * 4,
        out_specs=vmem(),
    )(color_terms, owner.reshape(-1, LANES), raw, mags, tab)

    zp, means, partial = pl.pallas_call(
        functools.partial(sweep_kernel, (tiles, bands, obs, stars, blocks, entries, fields, blk_rows, owned)),
        name="sweeps",
        out_shape=(
            jax.ShapeDtypeStruct((1, owned), F32),
            jax.ShapeDtypeStruct((1, stars), F32),
            jax.ShapeDtypeStruct((1, LANES), F32),
        ),
        in_specs=[smem()] + [vmem()] * 11,
        out_specs=(vmem(), vmem(), vmem()),
        scratch_shapes=[
            square,
            rows_state,
            rows_state,
            pltpu.VMEM((bands * entries * vrows // 2, LANES), F32),
            rows_state,
            pltpu.VMEM((bands * entries, LANES), F32),
            pltpu.VMEM((SWEEPS, vrows, LANES), F32),
            square,
            pltpu.VMEM((2 * groups, LANES, LANES), F32),
            pltpu.VMEM((2 * groups, SUBS, LANES), F32),
            rows_state,
            pltpu.VMEM((SWEEPS * bands, SUBS, LANES), F32),
            pltpu.VMEM((groups, 4 * bands, 2 * LANES), F32),
            rows_state,
            pltpu.VMEM((fields // LANES, LANES), F32),
        ],
        compiler_params=pltpu.CompilerParams(vmem_limit_bytes=20 * 1024 * 1024),
    )(limits, *late, *ready, same, keep)

    misfit = sky_sum(partial, bands, tiles)[0, :SWEEPS] / (obs * stars * tiles)
    return zp, means, misfit[:, None]


def fits_local(mesh, blocks_all, entries, stars, obs, bands, fields):
    tiles = mesh.shape["sky"]
    blocks = blocks_all // tiles
    return (
        2 * blocks_all == LANES
        and blocks == SUBS
        and bands == 4
        and bands * entries == LANES
        and obs == SUBS
        and 2 * bands == SUBS
        and mesh.shape["band"] == bands
        and stars // tiles == 2 * obs * LANES
        and (stars // blocks_all) % LANES == 0
        and fields % (SUBS * LANES) == 0
        and fields % (tiles * LANES) == 0
        and fields // SUBS + bands * LANES <= stars // tiles
    )


def from_behind(value, axis, steps):
    count = lax.axis_size(axis)
    pairs = [(source, (source + steps) % count) for source in range(count)]
    return lax.ppermute(value, axis, pairs)


def wide_body(magnitudes, weights, slots, block_fields, owner, colors, color_terms):
    band_count = color_terms.shape[0]
    tiles = lax.axis_size("sky")
    my_tile = lax.axis_index("sky")
    my_band = lax.axis_index("band")
    band_mags, band_wts, band_slots = (magnitudes, weights, slots)
    own_row = 0
    band_rows, obs_count, star_count = band_mags.shape
    block_count, list_len = block_fields.shape
    block_rows = star_count // block_count
    fields = owner.shape[0]
    slot_grid = band_slots.reshape(band_rows, obs_count, block_count, block_rows)
    entries = jnp.arange(list_len, dtype=jnp.int32)
    star_weight = jnp.sum(band_wts, axis=1)
    mixing = (
        jnp.eye(band_count, dtype=jnp.float32)
        + color_terms
        - jnp.diag(jnp.sum(color_terms, axis=1))
    )
    owner_order = jnp.argsort(owner, stable=True)
    owned = fields // tiles

    def slot_sums(values):
        grid = values.reshape(band_rows, obs_count, block_count, block_rows)
        hits = slot_grid[..., None] == entries
        return jnp.sum(jnp.where(hits, grid[..., None], 0.0), axis=(1, 3))

    def spread(list_vals):
        hits = slot_grid[..., None] == entries
        picked = jnp.sum(jnp.where(hits, list_vals[:, None, :, None, :], 0.0), axis=4)
        return picked.reshape(band_rows, obs_count, star_count)

    def predict(zp_obs):
        star_means = jnp.sum(band_wts * (band_mags - zp_obs), axis=1) / star_weight
        all_means = lax.all_gather(star_means, "band", axis=0, tiled=True)
        mix_row = lax.dynamic_index_in_dim(mixing, my_band, 0, keepdims=True)
        predicted = jnp.dot(mix_row, all_means, precision=lax.Precision.HIGHEST)
        return (star_means, predicted)

    positions = jnp.argsort(owner_order, stable=True)
    rank_in = positions - owner * owned
    live = block_fields < fields
    safe_ids = jnp.minimum(block_fields, fields - 1)
    relative = jnp.mod(jnp.take(owner, safe_ids) - my_tile + 1, tiles)
    list_ids = jnp.where(live, relative * owned + jnp.take(rank_in, safe_ids), 3 * owned)
    segments = 3 * owned
    nearby_idx = jnp.mod(my_tile + jnp.arange(3, dtype=jnp.int32) - 1, tiles)
    near_fields = jnp.take(owner_order.reshape(tiles, owned), nearby_idx, axis=0)
    zp_colors = jnp.take(colors, near_fields)[None]
    zero_pts = jnp.zeros((band_rows, 3, owned), jnp.float32)

    def flatten(table):
        return table.reshape(band_rows, 3 * owned)

    def combine(partial_flat):
        partial_sums = partial_flat.reshape(band_rows, 3, owned)
        from_left = from_behind(partial_sums[:, 1:3], "sky", 1)
        from_right = from_behind(partial_sums[:, 0:2], "sky", -1)
        far_left = from_behind(partial_sums[:, 2], "sky", 2)
        far_right = from_behind(partial_sums[:, 0], "sky", -2)
        below = far_left + from_left[:, 0] + partial_sums[:, 0]
        middle = from_left[:, 1] + partial_sums[:, 1] + from_right[:, 0]
        above = partial_sums[:, 2] + from_right[:, 1] + far_right
        return jnp.stack([below, middle, above], axis=1)

    def lookup(table):
        padded = jnp.concatenate([flatten(table), jnp.zeros((band_rows, 1), jnp.float32)], axis=1)
        return spread(jnp.take(padded, list_ids, axis=1))

    def segment_band(per_band):
        return jax.ops.segment_sum(
            per_band.reshape(-1), list_ids.reshape(-1), num_segments=segments + 1
        )[:segments]

    def totals(values):
        per_slot = slot_sums(values)
        return combine(jax.vmap(segment_band)(per_slot))

    denominators = totals(band_wts) + PRIOR_WEIGHT

    def squared_misfit(residual, zp_obs):
        per_band = jnp.sum(band_wts * (residual - zp_obs) ** 2, axis=(1, 2))
        return lax.dynamic_index_in_dim(per_band, own_row, 0, keepdims=False)

    def advance(table, color_no):
        zp_obs = lookup(table)
        _, predicted = predict(zp_obs)
        residual = band_mags - predicted[:, None, :]
        updated = totals(band_wts * residual) / denominators
        local_value = squared_misfit(residual, zp_obs)
        return (jnp.where(zp_colors == color_no, updated, table), local_value)

    def later_colors(color_no, table):
        return advance(table, color_no)[0]

    def record(local_value):
        return lax.psum(local_value, "sky")

    recorded = []
    for sweep_no in range(SWEEPS):
        zero_pts, local_value = advance(zero_pts, 0)
        if sweep_no > 0:
            recorded.append(record(local_value))
        zero_pts = lax.fori_loop(1, COLORS, later_colors, zero_pts)
    zp_obs = lookup(zero_pts)
    star_means, predicted = predict(zp_obs)
    residual = band_mags - predicted[:, None, :]
    recorded.append(record(squared_misfit(residual, zp_obs)))
    stacked = jnp.stack(recorded)
    misfit = stacked / (obs_count * star_count * tiles)
    own_zp = lax.dynamic_index_in_dim(zero_pts[:, 1], own_row, 0, keepdims=True)
    own_means = lax.dynamic_index_in_dim(star_means, own_row, 0, keepdims=True)
    return (own_zp, own_means, misfit[:, None])


def solution(mesh):
    in_specs = (
        P("band", None, "sky"),
        P("band", None, "sky"),
        P("band", None, "sky"),
        P("sky", None),
        P(),
        P(),
        P(),
    )
    out_specs = (P("band", "sky"), P("band", "sky"), P(None, "band"))

    def call(magnitudes, weights, slots, block_fields, owner, colors, color_terms):
        bands, obs, stars = magnitudes.shape
        blocks_all, entries = block_fields.shape
        local = fits_local(mesh, blocks_all, entries, stars, obs, bands, owner.shape[0])
        body = local_body if local else wide_body
        run = jax.shard_map(body, mesh=mesh, in_specs=in_specs, out_specs=out_specs, check_vma=False)
        return run(magnitudes, weights, slots, block_fields, owner, colors, color_terms)

    return call
```
